16 devices in a mesh: rep: 4 (over y, z, core), dp: 4 (over x).
Axes of the slice: x: 4, y: 2, z: 1, core: 2. Of those that a mesh axis runs over, the one named last changes fastest.
The devices are a block of a 4x4x8 slice.
Arguments:
- x: bfloat16 [16, 4096, 1024], P(('rep', 'dp')), parts along dimension 0
- dy: bfloat16 [16, 4096, 1024], P(('rep', 'dp')), parts along dimension 0
- w_gate: bfloat16 [2, 1024, 2816], replicated
- w_up: bfloat16 [2, 1024, 2816], replicated
- w_down: bfloat16 [2, 2816, 1024], replicated
- m_w_gate: float32 [2, 1024, 2816], P(None, 'dp')
- m_w_up: float32 [2, 1024, 2816], P(None, 'dp')
- m_w_down: float32 [2, 2816, 1024], P(None, 'dp')
- v_w_gate: float32 [2, 1024, 2816], P(None, 'dp')
- v_w_up: float32 [2, 1024, 2816], P(None, 'dp')
- v_w_down: float32 [2, 2816, 1024], P(None, 'dp')
Outputs:
- output 1: bfloat16 [8, 1024, 2816], P('rep'), parts along dimension 0
- output 2: bfloat16 [8, 1024, 2816], P('rep'), parts along dimension 0
- output 3: bfloat16 [8, 2816, 1024], P('rep'), parts along dimension 0
- output 4: float32 [8, 1024, 2816], P('rep', 'dp'), parts along dimension 0
- output 5: float32 [8, 1024, 2816], P('rep', 'dp'), parts along dimension 0
- output 6: float32 [8, 2816, 1024], P('rep', 'dp'), parts along dimension 0
- output 7: float32 [8, 1024, 2816], P('rep', 'dp'), parts along dimension 0
- output 8: float32 [8, 1024, 2816], P('rep', 'dp'), parts along dimension 0
- output 9: float32 [8, 2816, 1024], P('rep', 'dp'), parts along dimension 0
There are 4 independent parts. The reference program is written for one: setup_inputs(seed, part) draws one part's arguments, and reference() takes and returns one part's arrays. A program takes and returns all parts, laid end to end along the dimension named above; an argument that names none is the same for every part.
All inputs are finite; a program needn't handle non-finite values.
Results may differ from the reference program's by a relative error of at most 0.02.
Values are sent between devices in bfloat16 or wider.
A program may use at most 768 MiB of HBM per device.

```python
import jax
import jax.numpy as jnp
from jax import lax

SEQUENCES = 4
TOKENS = 4096
D = 1024
FF = 2816
LAYERS = 2
NAMES = ("w_gate", "w_up", "w_down")
SHAPES = {"w_gate": (LAYERS, D, FF), "w_up": (LAYERS, D, FF), "w_down": (LAYERS, FF, D)}


def bump(key, n, height):
    away = (jnp.arange(n, dtype=jnp.int32) - jax.random.randint(key, (), 0, n, jnp.int32)) % n
    return jnp.where(away < n // 8, height, 1.0)


def together(key, own, strength):
    shared = jax.random.normal(key, own.shape[1:], jnp.float32)
    return (own + strength * shared) * lax.rsqrt(1 + strength * strength)


def setup_inputs(seed: int = 0, part: int = 0) -> dict:
    kx, kdy, ka, kb, kz, kf, kh, kl, *keys = jax.random.split(jax.random.key(seed), 8 + 3 * len(NAMES))
    kx, kdy, ka, kb = (jax.random.fold_in(k, part) for k in (kx, kdy, ka, kb))
    kw, km, kv = (keys[i::3] for i in range(3))
    shape = (SEQUENCES, TOKENS, D)
    much_x, much_dy = jax.random.uniform(kz, (2,), jnp.float32, 0.0, 1.0)
    loud = 2.0 ** jax.random.uniform(jax.random.fold_in(kz, 1), (), jnp.float32, -1.0, 2.0)
    layers = 2.0 ** jax.random.uniform(kl, (LAYERS, 1, 1), jnp.float32, -1.0, 1.0)
    x = together(ka, jax.random.normal(kx, shape, jnp.float32), much_x) * bump(kf, D, 4.0)
    dy = together(kb, jax.random.normal(kdy, shape, jnp.float32), much_dy)
    drawn = {"x": x.astype(jnp.bfloat16), "dy": (loud * dy * (SEQUENCES * TOKENS) ** -0.5).astype(jnp.bfloat16)}
    for key, name in zip(kw, NAMES, strict=True):
        w = jax.random.normal(key, SHAPES[name], jnp.float32) * SHAPES[name][1] ** -0.5
        drawn[name] = (w * {"w_gate": 1.0, "w_up": bump(kh, FF, 4.0), "w_down": layers}[name]).astype(jnp.bfloat16)
    for key, name in zip(km, NAMES, strict=True):
        drawn[f"m_{name}"] = 0.1 * jax.random.normal(key, SHAPES[name], jnp.float32)
    for key, name in zip(kv, NAMES, strict=True):
        drawn[f"v_{name}"] = jax.random.uniform(key, SHAPES[name], jnp.float32, 0.005, 0.015)
    return drawn


def matmul(a, w):
    return jnp.dot(a, w, preferred_element_type=jnp.float32).astype(jnp.bfloat16)


def normed(h):
    wide = h.astype(jnp.float32)
    scale = lax.rsqrt(jnp.mean(wide**2, -1, keepdims=True) + 1e-6)
    return (wide * scale).astype(jnp.bfloat16)


def layer(h, w):
    a = normed(h)
    gate = jnp.dot(a, w["w_gate"], preferred_element_type=jnp.float32)
    up = jnp.dot(a, w["w_up"], preferred_element_type=jnp.float32)
    return h + matmul((jax.nn.silu(gate) * up).astype(jnp.bfloat16), w["w_down"])


def adamw(w, m, v, g):
    m = 0.9 * m + 0.1 * g
    v = 0.95 * v + 0.05 * g * g
    step = m * lax.rsqrt(v + 1e-8) + 0.1 * w
    return (w - 0.02 * step).astype(jnp.bfloat16), m, v


def stack(weights, h):
    return lax.scan(lambda h, w: (layer(h, w), None), h, weights)[0]


def reference(x, dy, w_gate, w_up, w_down, m_w_gate, m_w_up, m_w_down, v_w_gate, v_w_up, v_w_down):
    weights = dict(zip(NAMES, (w_gate, w_up, w_down), strict=True))

    def take(so_far, sequence):
        h, by_y = sequence
        _, back = jax.vjp(lambda w: stack(w, h), weights)
        return jax.tree.map(lambda total, term: total + term.astype(jnp.float32), so_far, back(by_y)[0]), None

    none_yet = {name: jnp.zeros(w.shape, jnp.float32) for name, w in weights.items()}
    by_weights, _ = lax.scan(take, none_yet, (x, dy))
    gradients = [by_weights[name].astype(jnp.bfloat16).astype(jnp.float32) for name in NAMES]
    new = [
        adamw(w.astype(jnp.float32), m, v, g)
        for w, m, v, g in zip((w_gate, w_up, w_down), (m_w_gate, m_w_up, m_w_down), (v_w_gate, v_w_up, v_w_down), gradients, strict=True)
    ]
    return tuple(one[which] for which in range(3) for one in new)
```

```python
import functools

import jax
import jax.numpy as jnp
from jax import lax
from jax.experimental import pallas as pl
from jax.experimental.pallas import tpu as pltpu
from jax.sharding import PartitionSpec as P

F32, BF16 = jnp.float32, jnp.bfloat16
BLOCK = 256
UNIT = 64
MIB = 2**20
TM = 512
ANY = pl.BlockSpec(memory_space=pl.ANY)


def dot(a, b):
    return jnp.dot(a, b, preferred_element_type=F32)


def norm_scale(wide):
    return lax.rsqrt(jnp.mean(wide * wide, -1, keepdims=True) + 1e-6)


def params(limit=60):
    return pltpu.CompilerParams(vmem_limit_bytes=limit * MIB, dimension_semantics=("arbitrary",))


def forward_kernel(blocks, x_ref, wg_hbm, wu_hbm, wd_hbm, a0_ref, h_ref, a1_ref, wg, wu, wd, act, sems):
    step = pl.program_id(0)

    def copies(b):
        cols = pl.ds(b * BLOCK, BLOCK)
        return (
            pltpu.make_async_copy(wg_hbm.at[0, :, cols], wg.at[:, cols], sems.at[0, b]),
            pltpu.make_async_copy(wu_hbm.at[0, :, cols], wu.at[:, cols], sems.at[1, b]),
            pltpu.make_async_copy(wd_hbm.at[0, cols, :], wd.at[cols, :], sems.at[2, b]),
        )

    @pl.when(step == 0)
    def _():
        for b in range(blocks):
            for c in copies(b):
                c.start()

    wide = x_ref[...].astype(F32)
    a0_ref[...] = (wide * norm_scale(wide)).astype(BF16)

    @pl.when(step == 0)
    def _():
        for b in range(blocks):
            for c in copies(b):
                c.wait()

    for b in range(blocks):
        cols = slice(b * BLOCK, (b + 1) * BLOCK)
        gate = dot(a0_ref[...], wg[:, cols])
        up = dot(a0_ref[...], wu[:, cols])
        act[:, cols] = (gate * jax.nn.sigmoid(gate) * up).astype(BF16)
    h = x_ref[...] + dot(act[...], wd[...]).astype(BF16)
    h_ref[...] = h
    wide = h.astype(F32)
    a1_ref[...] = (wide * norm_scale(wide)).astype(BF16)


def forward(x, wg, wu, wd, tm=None):
    tm = tm or TM
    t, d = x.shape
    ff = wg.shape[-1]
    blocks = ff // BLOCK
    tile = pl.BlockSpec((tm, d), lambda i: (i, 0))
    return pl.pallas_call(
        functools.partial(forward_kernel, blocks),
        grid=(t // tm,),
        in_specs=[tile, ANY, ANY, ANY],
        out_specs=[tile] * 3,
        out_shape=[jax.ShapeDtypeStruct((t, d), BF16)] * 3,
        scratch_shapes=[
            pltpu.VMEM((d, ff), BF16),
            pltpu.VMEM((d, ff), BF16),
            pltpu.VMEM((ff, d), BF16),
            pltpu.VMEM((tm, ff), BF16),
            pltpu.SemaphoreType.DMA((3, blocks)),
        ],
        compiler_params=params(),
        cost_estimate=pl.CostEstimate(flops=6 * t * d * ff, bytes_accessed=8 * t * d + 6 * d * ff, transcendentals=t * ff),
        name="forward",
    )(x, wg, wu, wd)


def adamw(w, m, v, g):
    m = 0.9 * m + 0.1 * g
    v = 0.95 * v + 0.05 * g * g
    step = m * lax.rsqrt(v + 1e-8) + 0.1 * w
    return (w - 0.02 * step).astype(BF16), m, v


GU, DOWN, LAST = 0, 1, 2
RING = 4
PACKS = 17


def pack_kind(p):
    r = lax.rem(p, PACKS)
    down = ((r >= 4) & (r < 6)) | ((r >= 10) & (r < 12))
    last = r >= 15
    return {GU: jnp.logical_not(down | last), DOWN: down, LAST: last}


def backward_kernel(
    n, steps, d, ff, axis,
    a1_hbm, dy_hbm, h1_hbm, a0_hbm, wg_hbm, wu_hbm, wd_hbm, mg_hbm, mu_hbm, md_hbm, vg_hbm, vu_hbm, vd_hbm,
    ng_hbm, nu_hbm, nd_hbm, mg_out, mu_out, md_out, vg_out, vu_out, vd_out, dh_hbm,
    tiles, at, dht, wgu, wdn, wdt, wgut, accgu, accd, da, dbuf, hout,
    send, keep, own, r1, r2, s2, wnew, mvin, win, mvout,
    tile_sem, weight_sem, hout_sem, s1s, s1r, s2s, s2r, g1s, g1r, g2s, g2r, loc_sem, mvin_sem, mvout_sem,
):
    tm = tiles.shape[2]
    blocks = ff // BLOCK
    q = BLOCK
    me = lax.axis_index(axis)
    right, left, far = (lax.rem(me + k, n) for k in (1, n - 1, 2))
    to = ({axis: right}, {axis: left})
    mult = pl.multiple_of

    barrier = pltpu.get_barrier_semaphore()
    for dev in to:
        pl.semaphore_signal(barrier, inc=1, device_id=dev, device_id_type=pl.DeviceIdType.MESH)
    pl.semaphore_wait(barrier, 2)


    def layer_of(p):
        return 1 - p // PACKS

    def gu_cols(p):
        r = lax.rem(p, PACKS)
        i = jnp.where(r < 4, r, jnp.where(r < 10, r - 2, r - 4))
        return mult((3 * lax.rem(i, 4) + i // 4) * q, q)

    def down_cols(kind, p, half):
        r = lax.rem(p, PACKS)
        first = r - 15 if kind == LAST else jnp.where(r < 6, r - 4, r - 10)
        return mult((2 * first + half) * q, q)

    def down_row(p, dev):
        r = lax.rem(p, PACKS)
        return mult(jnp.where(r < 6, 0, 4 * UNIT) + dev * UNIT, UNIT)

    def last_row(dev, u):
        return mult(jnp.where(u < dev, u, 8 + u) * UNIT, UNIT)

    def height(kind):
        return 3 * UNIT if kind == LAST else q

    def rows_in(kind, p, dev, half, ref_gu, ref_d, per_device):
        lay = layer_of(p)
        if kind == GU:
            base = 0 if per_device else mult(dev * q, q)
            return [(ref_gu[half].at[lay, pl.ds(base, q), pl.ds(gu_cols(p), q)], 0, q)]
        cols = pl.ds(down_cols(kind, p, half), q)
        base = 0 if per_device else dev * (ff // n)
        if kind == DOWN:
            return [(ref_d.at[lay, pl.ds(mult(base + down_row(p, dev), UNIT), q), cols], 0, q)]
        return [(ref_d.at[lay, pl.ds(mult(base + last_row(dev, u), UNIT), UNIT), cols], u * UNIT, UNIT) for u in range(3)]

    def new_pieces(kind, p, dev, half):
        return rows_in(kind, p, dev, half, (ng_hbm, nu_hbm), nd_hbm, False)


    def s1_copy(kind, p, way):
        s, h = lax.rem(p, RING), height(kind)
        rows = pl.ds(0, 2 * h)
        return pltpu.make_async_remote_copy(
            send.at[s, way, rows], r1.at[s, way, rows], s1s.at[way, s], s1r.at[way, s], to[way], pl.DeviceIdType.MESH
        )

    def s2_copy(kind, p, way):
        s, h = lax.rem(p, RING), height(kind)
        rows = pl.ds(0, h)
        return pltpu.make_async_remote_copy(
            s2.at[s, way, rows], r2.at[s, way, rows], s2s.at[way, s], s2r.at[way, s], to[way], pl.DeviceIdType.MESH
        )

    def g1_copies(kind, p, way, half):
        s = lax.rem(p, RING)
        return [
            pltpu.make_async_remote_copy(
                wnew.at[s, half, pl.ds(at_, size)], view, g1s.at[way, half, s], g1r.at[way, half, s], to[way], pl.DeviceIdType.MESH
            )
            for view, at_, size in new_pieces(kind, p, me, half)
        ]

    def g2_copies(kind, p, way):
        s, dev = lax.rem(p, 2 * RING), (left, right)[way]
        return [
            pltpu.make_async_remote_copy(view, view, g2s.at[way, s], g2r.at[way, s], to[way], pl.DeviceIdType.MESH)
            for view, _, _ in new_pieces(kind, p, dev, way)
        ]

    def total_of(kind, p, way, half, sems, side):
        s, h = lax.rem(p, RING), height(kind)
        ref = wnew.at[s, half, pl.ds(0, h)]
        copy = pltpu.make_async_remote_copy(ref, ref, sems[0], sems[1], to[way], pl.DeviceIdType.MESH)
        copy.wait_send() if side == 0 else copy.wait_recv()

    def moment_loads(kind, p):
        b, s = lax.rem(p, 2), []
        for half in range(2):
            for k, (gu, dn) in enumerate((((mg_hbm, mu_hbm), md_hbm), ((vg_hbm, vu_hbm), vd_hbm))):
                for view, at_, size in rows_in(kind, p, me, half, gu, dn, True):
                    s.append(pltpu.make_async_copy(view, mvin.at[b, 2 * half + k, pl.ds(at_, size)], mvin_sem.at[b, 2 * half + k]))
            for view, at_, size in rows_in(kind, p, me, half, (wg_hbm, wu_hbm), wd_hbm, False):
                s.append(pltpu.make_async_copy(view, win.at[b, half, pl.ds(at_, size)], mvin_sem.at[b, 4 + half]))
        return s

    def moment_loads_wait(kind, p):
        b, rows = lax.rem(p, 2), pl.ds(0, height(kind))
        for k in range(4):
            pltpu.make_async_copy(mvin.at[b, k, rows], mvin.at[b, k, rows], mvin_sem.at[b, k]).wait()
        for half in range(2):
            pltpu.make_async_copy(win.at[b, half, rows], win.at[b, half, rows], mvin_sem.at[b, 4 + half]).wait()

    def moment_stores(kind, p):
        b, s = lax.rem(p, 2), []
        for half in range(2):
            for k, (gu, dn) in enumerate((((mg_out, mu_out), md_out), ((vg_out, vu_out), vd_out))):
                for view, at_, size in rows_in(kind, p, me, half, gu, dn, True):
                    s.append(pltpu.make_async_copy(mvout.at[b, 2 * half + k, pl.ds(at_, size)], view, mvout_sem.at[b, 2 * half + k]))
        return s

    def moment_stores_wait(kind, p):
        b, rows = lax.rem(p, 2), pl.ds(0, height(kind))
        for k in range(4):
            pltpu.make_async_copy(mvout.at[b, k, rows], mvout.at[b, k, rows], mvout_sem.at[b, k]).wait()

    def own_copies(kind, p):
        s = lax.rem(p, RING)
        return [
            pltpu.make_async_copy(wnew.at[s, half, pl.ds(at_, size)], view, loc_sem.at[half, s])
            for half in range(2)
            for view, at_, size in new_pieces(kind, p, me, half)
        ]

    def stage(kind, p):
        s, h = lax.rem(p, RING), height(kind)
        if kind == GU:
            def part(dev, half):
                return accgu[pl.ds(mult(dev * q, q), q), half * q : (half + 1) * q].astype(BF16)
        else:
            def part(dev, half):
                return dbuf[pl.ds(mult(dev * h, UNIT), h), pl.ds(down_cols(kind, p, half), q)]
        send[s, 0, :h, :] = part(far, 0)
        send[s, 0, h : 2 * h, :] = part(right, 1)
        send[s, 1, :h, :] = part(far, 1)
        send[s, 1, h : 2 * h, :] = part(left, 0)
        keep[s, 0, :h, :] = part(right, 0)
        keep[s, 1, :h, :] = part(left, 1)
        own[s, 0, :h, :] = part(me, 0)
        own[s, 1, :h, :] = part(me, 1)

    def do_s1(kind, p):
        stage(kind, p)
        for c in moment_loads(kind, p):
            c.start()
        for way in range(2):
            s1_copy(kind, p, way).start()

    def do_s2(kind, p):
        s, h = lax.rem(p, RING), height(kind)
        for way in range(2):
            s1_copy(kind, p, way).wait_recv()
            s2[s, way, :h, :] = (keep[s, way, :h, :].astype(F32) + r1[s, way, :h, :].astype(F32)).astype(BF16)
            s2_copy(kind, p, way).start()

    def do_s3(kind, p):
        s, b, h = lax.rem(p, RING), lax.rem(p, 2), height(kind)
        moment_loads_wait(kind, p)
        for k, cond in pack_kind(p - 2).items():
            @pl.when(cond & (p >= 2))
            def _():
                moment_stores_wait(k, p - 2)
        for way in range(2):
            s2_copy(kind, p, way).wait_recv()

        def rows_of(u, _):
            rows = pl.ds(mult(u * UNIT, UNIT), UNIT)
            rest = pl.ds(mult(h + u * UNIT, UNIT), UNIT)
            for half in range(2):
                g = own[s, half, rows, :].astype(F32) + r1[s, 1 - half, rest, :].astype(F32) + r2[s, half, rows, :].astype(F32)
                g = g.astype(BF16).astype(F32)
                w, m, v = adamw(win[b, half, rows, :].astype(F32), mvin[b, 2 * half, rows, :], mvin[b, 2 * half + 1, rows, :], g)
                wnew[s, half, rows, :] = w
                mvout[b, 2 * half, rows, :] = m
                mvout[b, 2 * half + 1, rows, :] = v
            return 0

        lax.fori_loop(0, h // UNIT, rows_of, 0)
        for c in moment_stores(kind, p):
            c.start()
        for way in range(2):
            for half in ((0, 1), (1, 0))[way]:
                for c in g1_copies(kind, p, way, half):
                    c.start()
        for c in own_copies(kind, p):
            c.start()

    def do_s4(kind, p):
        s = lax.rem(p, RING)
        for way in range(2):
            s1_copy(kind, p, way).wait_send()
            s2_copy(kind, p, way).wait_send()
            for half in ((0, 1), (1, 0))[way]:
                total_of(kind, p, way, half, (g1s.at[way, half, s], g1r.at[way, half, s]), 1)
                if half == way:
                    for c in g2_copies(kind, p, way):
                        c.start()

    def do_s5(kind, p):
        s, rows = lax.rem(p, RING), pl.ds(0, height(kind))
        for way in range(2):
            for half in range(2):
                total_of(kind, p, way, half, (g1s.at[way, half, s], g1r.at[way, half, s]), 0)
            far_s = lax.rem(p, 2 * RING)
            total_of(kind, p, way, way, (g2s.at[way, far_s], g2r.at[way, far_s]), 1)
            total_of(kind, p, way, way, (g2s.at[way, far_s], g2r.at[way, far_s]), 0)
        for half in range(2):
            pltpu.make_async_copy(wnew.at[s, half, rows], wnew.at[s, half, rows], loc_sem.at[half, s]).wait()

    def each(do, p, among=(GU, DOWN, LAST)):
        for kind, cond in pack_kind(p).items():
            if kind in among:
                @pl.when(cond & (p >= 0) & (p < 2 * PACKS))
                def _():
                    do(kind, p)

    def full(p, among=(GU, DOWN, LAST)):
        each(do_s1, p, among)
        each(do_s3, p - 1)

    def half(p):
        each(do_s2, p)
        each(do_s4, p - 2)
        each(do_s5, p - 4)


    def weight_loads(it):
        b, lay = lax.rem(it, 2), 1 - it // blocks
        i = lax.rem(it, blocks)
        cols = pl.ds(mult((3 * lax.rem(i, 4) + i // 4) * q, q), q)
        return (
            pltpu.make_async_copy(wg_hbm.at[lay, :, cols], wgu.at[b, :, pl.ds(0, q)], weight_sem.at[b, 0]),
            pltpu.make_async_copy(wu_hbm.at[lay, :, cols], wgu.at[b, :, pl.ds(q, q)], weight_sem.at[b, 1]),
            pltpu.make_async_copy(wd_hbm.at[lay, cols, :], wdn.at[b], weight_sem.at[b, 2]),
        )

    def tile_loads(a_hbm, d_hbm, t):
        b, rows = lax.rem(t, 2), pl.ds(mult(t * tm, tm), tm)
        return (
            pltpu.make_async_copy(a_hbm.at[rows, :], tiles.at[b, 0], tile_sem.at[b, 0]),
            pltpu.make_async_copy(d_hbm.at[rows, :], tiles.at[b, 1], tile_sem.at[b, 1]),
        )

    def start_tile(layer_1, t):
        @pl.when(layer_1)
        def _():
            for c in tile_loads(a1_hbm, dy_hbm, t):
                c.start()

        @pl.when(jnp.logical_not(layer_1))
        def _():
            for c in tile_loads(a0_hbm, dh_hbm, t):
                c.start()

    def compute(b, wb, t, layer_1):
        a, dh = tiles[b, 0], tiles[b, 1]
        at[...] = a.T
        dht[...] = dh.T
        gu = dot(a, wgu[wb])
        dact = dot(dh, wdt[...]).astype(BF16).astype(F32)
        gate, up = gu[:, :q], gu[:, q:]
        s = jax.nn.sigmoid(gate)
        silu = gate * s
        act = (silu * up).astype(BF16)
        dup = (dact * silu).astype(BF16)
        dgate = (dact * up * (s + silu * (1 - s))).astype(BF16)
        dgu = jnp.concatenate([dgate, dup], -1)
        accgu[...] += dot(at[...], dgu)
        accd[...] += dot(dht[...], act)
        if layer_1:
            rows = pl.ds(mult(t * tm, tm), tm)
            da[rows, :] += dot(dgu, wgut[...])

    def between_layers():
        def loads(t):
            return tile_loads(h1_hbm, dy_hbm, t)

        def store(t):
            return pltpu.make_async_copy(hout.at[lax.rem(t, 2)], dh_hbm.at[pl.ds(mult(t * tm, tm), tm), :], hout_sem.at[lax.rem(t, 2)])

        for c in loads(0):
            c.start()

        def tile(t, _):
            @pl.when(t + 1 < steps)
            def _():
                for c in loads(t + 1):
                    c.start()

            for c in loads(t):
                c.wait()

            @pl.when(t >= 2)
            def _():
                store(t - 2).wait()

            b = lax.rem(t, 2)
            g = da[pl.ds(mult(t * tm, tm), tm), :].astype(BF16).astype(F32)
            wide = tiles[b, 0].astype(F32)
            scale = norm_scale(wide)
            inner = jnp.mean(g * wide, -1, keepdims=True)
            hout[b] = tiles[b, 1] + (scale * g - wide * (scale * scale * scale * inner)).astype(BF16)
            store(t).start()
            return 0

        lax.fori_loop(0, steps, tile, 0)
        store(steps - 2).wait()
        store(steps - 1).wait()

    for c in weight_loads(0):
        c.start()
    start_tile(True, 0)
    da[...] = jnp.zeros_like(da)

    def block(it, _):
        layer_1 = it < blocks
        wb, i = lax.rem(it, 2), lax.rem(it, blocks)
        ends_group = (i == 3) | (i == 7) | (i == blocks - 1)
        after_group = (i == 4) | (i == 8) | (it == blocks)
        p = PACKS * (it // blocks) + i + 2 * (i // 4)
        before = it - 1
        bi = lax.rem(before + blocks, blocks)
        prev = PACKS * (before // blocks) + bi + 2 * (bi // 4)

        @pl.when(it == blocks)
        def _():
            between_layers()
            start_tile(False, 0)

        for c in weight_loads(it):
            c.wait()

        @pl.when(it + 1 < 2 * blocks)
        def _():
            for c in weight_loads(it + 1):
                c.start()

        wdt[...] = wdn[wb].T

        @pl.when(layer_1)
        def _():
            wgut[...] = wgu[wb].T

        accgu[...] = jnp.zeros_like(accgu)
        accd[...] = jnp.zeros_like(accd)

        def tile(t, _):
            b = lax.rem(t, 2)
            for c in tile_loads(a1_hbm, dy_hbm, t):
                c.wait()

            more = (t + 1 < steps) | ((it + 1 != blocks) & (it + 1 != 2 * blocks))

            @pl.when(more)
            def _():
                start_tile(layer_1, lax.rem(t + 1, steps))

            @pl.when(layer_1)
            def _():
                compute(b, wb, t, True)

            @pl.when(jnp.logical_not(layer_1))
            def _():
                compute(b, wb, t, False)

            @pl.when((t == 1) & (it >= 1))
            def _():
                half(prev)

                @pl.when(after_group)
                def _():
                    full(prev + 1, (DOWN, LAST))

            @pl.when((t == 3) & after_group)
            def _():
                half(prev + 1)
                full(prev + 2, (DOWN, LAST))

            @pl.when((t == 5) & after_group)
            def _():
                half(prev + 2)

            return 0

        lax.fori_loop(0, steps, tile, 0)
        k = lax.rem(i, 4)
        for c in range(d // q):
            dbuf[pl.ds(mult(k * q, q), q), c * q : (c + 1) * q] = accd[c * q : (c + 1) * q, :].astype(BF16).T
        full(p, (GU,))
        return 0

    lax.fori_loop(0, 2 * blocks, block, 0)
    end = 2 * PACKS

    def tail(p, _):
        half(p)
        full(p + 1, (DOWN, LAST))
        return 0

    lax.fori_loop(end - 3, end, tail, 0)

    def drain(p, _):
        each(do_s4, p - 2)
        each(do_s5, p - 4)
        return 0

    lax.fori_loop(end, end + 4, drain, 0)
    for p in (end - 2, end - 1):
        moment_stores_wait(LAST, p)


def backward(a1, dy, h1, a0, wg, wu, wd, moments, n, axis, tm=None):
    tm = tm or TM
    t, d = dy.shape
    ff = wg.shape[-1]
    q = BLOCK
    V = pltpu.VMEM
    DMA = pltpu.SemaphoreType.DMA
    mg, mu, md, vg, vu, vd = moments
    outs = [jax.ShapeDtypeStruct(w.shape, BF16) for w in (wg, wu, wd)]
    outs += [jax.ShapeDtypeStruct(m.shape, F32) for m in moments]
    outs += [jax.ShapeDtypeStruct((t, d), BF16)]
    return pl.pallas_call(
        functools.partial(backward_kernel, n, t // tm, d, ff, axis),
        in_specs=[ANY] * 13,
        out_specs=[ANY] * 10,
        out_shape=outs,
        scratch_shapes=[
            V((2, 2, tm, d), BF16),
            V((d, tm), BF16),
            V((d, tm), BF16),
            V((2, d, 2 * q), BF16),
            V((2, q, d), BF16),
            V((d, q), BF16),
            V((2 * q, d), BF16),
            V((d, 2 * q), F32),
            V((d, q), F32),
            V((t, d), F32),
            V((4 * q, d), BF16),
            V((2, tm, d), BF16),
            V((RING, 2, 2 * q, q), BF16),
            V((RING, 2, q, q), BF16),
            V((RING, 2, q, q), BF16),
            V((RING, 2, 2 * q, q), BF16),
            V((RING, 2, q, q), BF16),
            V((RING, 2, q, q), BF16),
            V((RING, 2, q, q), BF16),
            V((2, 4, q, q), F32),
            V((2, 2, q, q), BF16),
            V((2, 4, q, q), F32),
            DMA((2, 2)),
            DMA((2, 3)),
            DMA((2,)),
            DMA((2, RING)),
            DMA((2, RING)),
            DMA((2, RING)),
            DMA((2, RING)),
            DMA((2, 2, RING)),
            DMA((2, 2, RING)),
            DMA((2, 2 * RING)),
            DMA((2, 2 * RING)),
            DMA((2, RING)),
            DMA((2, 6)),
            DMA((2, 4)),
        ],
        compiler_params=pltpu.CompilerParams(vmem_limit_bytes=62 * MIB, collective_id=0, has_side_effects=True),
        cost_estimate=pl.CostEstimate(flops=28 * t * d * ff, bytes_accessed=44 * t * d, transcendentals=2 * t * ff),
        name="backward",
    )(a1, dy, h1, a0, wg, wu, wd, *moments)


def solution(mesh):
    n = mesh.shape["dp"]

    def step(x, dy, wg, wu, wd, m_g, m_u, m_d, v_g, v_u, v_d):
        x, dy = x[0], dy[0]
        a0, h1, a1 = forward(x, wg, wu, wd)
        return backward(a1, dy, h1, a0, wg, wu, wd, (m_g, m_u, m_d, v_g, v_u, v_d), n, "dp")[:9]

    seq = P(("rep", "dp"), None, None)
    rows = P(None, "dp", None)
    whole = P("rep", None, None)
    part = P("rep", "dp", None)
    return jax.shard_map(
        step,
        mesh=mesh,
        in_specs=(seq, seq, P(), P(), P()) + (rows,) * 6,
        out_specs=(whole,) * 3 + (part,) * 6,
        check_vma=False,
    )
```

```python
import functools

import jax
import jax.numpy as jnp
from jax import lax
from jax.experimental import pallas as pl
from jax.experimental.pallas import tpu as pltpu
from jax.sharding import PartitionSpec as P

F32, BF16 = jnp.float32, jnp.bfloat16
BLOCK = 256
UNIT = 64
MIB = 2**20
TM = 512
ANY = pl.BlockSpec(memory_space=pl.ANY)


def dot(a, b):
    return jnp.dot(a, b, preferred_element_type=F32)


def norm_scale(wide):
    return lax.rsqrt(jnp.mean(wide * wide, -1, keepdims=True) + 1e-6)


def params(limit=60):
    return pltpu.CompilerParams(vmem_limit_bytes=limit * MIB, dimension_semantics=("arbitrary",))


def forward_kernel(blocks, x_ref, wg_hbm, wu_hbm, wd_hbm, a0_ref, h_ref, a1_ref, wg, wu, wd, act, sems):
    step = pl.program_id(0)

    def copies(b):
        cols = pl.ds(b * BLOCK, BLOCK)
        return (
            pltpu.make_async_copy(wg_hbm.at[0, :, cols], wg.at[:, cols], sems.at[0, b]),
            pltpu.make_async_copy(wu_hbm.at[0, :, cols], wu.at[:, cols], sems.at[1, b]),
            pltpu.make_async_copy(wd_hbm.at[0, cols, :], wd.at[cols, :], sems.at[2, b]),
        )

    @pl.when(step == 0)
    def _():
        for b in range(blocks):
            for c in copies(b):
                c.start()

    wide = x_ref[...].astype(F32)
    a0_ref[...] = (wide * norm_scale(wide)).astype(BF16)

    @pl.when(step == 0)
    def _():
        for b in range(blocks):
            for c in copies(b):
                c.wait()

    for b in range(blocks):
        cols = slice(b * BLOCK, (b + 1) * BLOCK)
        gate = dot(a0_ref[...], wg[:, cols])
        up = dot(a0_ref[...], wu[:, cols])
        act[:, cols] = (gate * jax.nn.sigmoid(gate) * up).astype(BF16)
    h = x_ref[...] + dot(act[...], wd[...]).astype(BF16)
    h_ref[...] = h
    wide = h.astype(F32)
    a1_ref[...] = (wide * norm_scale(wide)).astype(BF16)


def forward(x, wg, wu, wd, tm=None):
    tm = tm or TM
    t, d = x.shape
    ff = wg.shape[-1]
    blocks = ff // BLOCK
    tile = pl.BlockSpec((tm, d), lambda i: (i, 0))
    return pl.pallas_call(
        functools.partial(forward_kernel, blocks),
        grid=(t // tm,),
        in_specs=[tile, ANY, ANY, ANY],
        out_specs=[tile] * 3,
        out_shape=[jax.ShapeDtypeStruct((t, d), BF16)] * 3,
        scratch_shapes=[
            pltpu.VMEM((d, ff), BF16),
            pltpu.VMEM((d, ff), BF16),
            pltpu.VMEM((ff, d), BF16),
            pltpu.VMEM((tm, ff), BF16),
            pltpu.SemaphoreType.DMA((3, blocks)),
        ],
        compiler_params=params(),
        cost_estimate=pl.CostEstimate(flops=6 * t * d * ff, bytes_accessed=8 * t * d + 6 * d * ff, transcendentals=t * ff),
        name="forward",
    )(x, wg, wu, wd)


def adamw(w, m, v, g):
    m = 0.9 * m + 0.1 * g
    v = 0.95 * v + 0.05 * g * g
    step = m * lax.rsqrt(v + 1e-8) + 0.1 * w
    return (w - 0.02 * step).astype(BF16), m, v


GU, DOWN, LAST = 0, 1, 2
RING = 6
LEAD = 4
QUARTERS = 4
GROUPS = 3
KEPT = 11
SLOTS = 12
AHEAD = 6


def pack_of_block(it):
    return jnp.where(it < LEAD, it, 2 * it - LEAD + 1)


def pack_kind(p, blocks):
    paired = (p >= LEAD) & (p < 4 * blocks - LEAD)
    down = (paired & (lax.rem(p, 2) == 0)) | (p >= 4 * blocks - LEAD)
    last = down & (lax.rem(pack_down(p, blocks) // QUARTERS, GROUPS) == GROUPS - 1)
    return {GU: jnp.logical_not(down), DOWN: down & jnp.logical_not(last), LAST: last}


def pack_block(p):
    return jnp.where(p < LEAD, p, (p + LEAD - 1) // 2)


def pack_down(p, blocks):
    return jnp.where(p < 4 * blocks - LEAD, jnp.maximum(p - LEAD, 0) // 2, p - 2 * blocks)


def backward_kernel(
    n, steps, d, ff, axis,
    a1_hbm, dy_hbm, h1_hbm, a0_hbm, wg_hbm, wu_hbm, wd_hbm, mg_hbm, mu_hbm, md_hbm, vg_hbm, vu_hbm, vd_hbm,
    ng_hbm, nu_hbm, nd_hbm, mg_out, mu_out, md_out, vg_out, vu_out, vd_out, dh_hbm, kept_a, kept_b,
    tiles, at, dht, wgu, wdn, wdt, wgut, accgu, accd, da, dbuf, hout,
    send, keep, own, r1, r2, s2, wnew, mvin, win, mvout,
    tile_sem, weight_sem, hout_sem, s1s, s1r, s2s, s2r, g1s, g1r, g2s, g2r, loc_sem, mvin_sem, mvout_sem,
):
    tm = tiles.shape[2]
    blocks = ff // BLOCK
    packs = 2 * blocks + 2 * GROUPS * QUARTERS
    q = BLOCK
    me = lax.axis_index(axis)
    right, left, far = (lax.rem(me + k, n) for k in (1, n - 1, 2))
    to = ({axis: right}, {axis: left})
    mult = pl.multiple_of

    barrier = pltpu.get_barrier_semaphore()
    for dev in to:
        pl.semaphore_signal(barrier, inc=1, device_id=dev, device_id_type=pl.DeviceIdType.MESH)
    pl.semaphore_wait(barrier, 2)


    kind_of = functools.partial(pack_kind, blocks=blocks)

    def block_cols(it):
        i = lax.rem(it, blocks)
        return mult((3 * lax.rem(i, 4) + i // 4) * q, q)

    def down_group(p):
        return pack_down(p, blocks) // QUARTERS

    def down_cols(p):
        return mult(lax.rem(pack_down(p, blocks), QUARTERS) * q, q)

    def height(kind):
        return {GU: q, DOWN: q // 2, LAST: 3 * UNIT // 2}[kind]

    def last_row(dev, k):
        u = k // 2
        return mult(jnp.where(u < dev, u * UNIT, 8 * UNIT + u * UNIT) + (k % 2) * (UNIT // 2), UNIT // 2)

    def rows_in(kind, p, dev, half, ref_gu, ref_d, per_device):
        if kind == GU:
            it = pack_block(p)
            base = 0 if per_device else mult(dev * q, q)
            return [(ref_gu[half].at[1 - it // blocks, pl.ds(base, q), pl.ds(block_cols(it), q)], 0, q)]
        group = down_group(p)
        lay, cols = 1 - group // GROUPS, pl.ds(down_cols(p), q)
        base = 0 if per_device else dev * (ff // n)
        if kind == DOWN:
            row = base + lax.rem(group, GROUPS) * 4 * UNIT + dev * UNIT + half * (q // 2)
            return [(ref_d.at[lay, pl.ds(mult(row, UNIT), q // 2), cols], 0, q // 2)]
        small = UNIT // 2
        return [
            (ref_d.at[lay, pl.ds(mult(base + last_row(dev, 3 * half + k), small), small), cols], k * small, small) for k in range(3)
        ]

    def kept_rows(kind, p):
        k = p - (packs - KEPT)
        pair, small = q + q // 2, 3 * UNIT // 2
        row = {
            GU: k // 2 * pair,
            DOWN: jnp.where(k < 5, k // 2 * pair + q, 2 * pair + q + (k - 5) * (q // 2)),
            LAST: 3 * pair + q // 2 + (k - 7) * small,
        }[kind]
        return pl.ds(mult(row, UNIT // 2), height(kind))

    def new_pieces(kind, p, dev, half):
        return rows_in(kind, p, dev, half, (ng_hbm, nu_hbm), nd_hbm, False)


    def s1_copy(kind, p, way):
        s, h = lax.rem(p, RING), height(kind)
        rows = pl.ds(0, 2 * h)
        return pltpu.make_async_remote_copy(
            send.at[s, way, rows], r1.at[s, way, rows], s1s.at[way, s], s1r.at[way, s], to[way], pl.DeviceIdType.MESH
        )

    def s2_copy(kind, p, way):
        s, h = lax.rem(p, RING), height(kind)
        rows = pl.ds(0, h)
        return pltpu.make_async_remote_copy(
            s2.at[s, way, rows], r2.at[s, way, rows], s2s.at[way, s], s2r.at[way, s], to[way], pl.DeviceIdType.MESH
        )

    def g1_copies(kind, p, way, half):
        s = lax.rem(p, RING)
        return [
            pltpu.make_async_remote_copy(
                wnew.at[s, half, pl.ds(at_, size)], view, g1s.at[way, half, s], g1r.at[way, half, s], to[way], pl.DeviceIdType.MESH
            )
            for view, at_, size in new_pieces(kind, p, me, half)
        ]

    def g2_copies(kind, p, way):
        s, dev = lax.rem(p, 2 * RING), (left, right)[way]
        return [
            pltpu.make_async_remote_copy(view, view, g2s.at[way, s], g2r.at[way, s], to[way], pl.DeviceIdType.MESH)
            for view, _, _ in new_pieces(kind, p, dev, way)
        ]

    def total_of(kind, p, way, half, sems, side):
        s, h = lax.rem(p, RING), height(kind)
        ref = wnew.at[s, half, pl.ds(0, h)]
        copy = pltpu.make_async_remote_copy(ref, ref, sems[0], sems[1], to[way], pl.DeviceIdType.MESH)
        copy.wait_send() if side == 0 else copy.wait_recv()

    def moment_loads(kind, p):
        b, s = lax.rem(p, 2), []
        for half in range(2):
            for k, (gu, dn) in enumerate((((mg_hbm, mu_hbm), md_hbm), ((vg_hbm, vu_hbm), vd_hbm))):
                for view, at_, size in rows_in(kind, p, me, half, gu, dn, True):
                    s.append(pltpu.make_async_copy(view, mvin.at[b, 2 * half + k, pl.ds(at_, size)], mvin_sem.at[b, 2 * half + k]))
            for view, at_, size in rows_in(kind, p, me, half, (wg_hbm, wu_hbm), wd_hbm, False):
                s.append(pltpu.make_async_copy(view, win.at[b, half, pl.ds(at_, size)], mvin_sem.at[b, 4 + half]))
        return s

    def moment_loads_wait(kind, p):
        b, rows = lax.rem(p, 2), pl.ds(0, height(kind))
        for k in range(4):
            pltpu.make_async_copy(mvin.at[b, k, rows], mvin.at[b, k, rows], mvin_sem.at[b, k]).wait()
        for half in range(2):
            pltpu.make_async_copy(win.at[b, half, rows], win.at[b, half, rows], mvin_sem.at[b, 4 + half]).wait()

    def moment_stores(kind, p):
        b, s = lax.rem(p, 2), []
        for half in range(2):
            for k, (gu, dn) in enumerate((((mg_out, mu_out), md_out), ((vg_out, vu_out), vd_out))):
                for view, at_, size in rows_in(kind, p, me, half, gu, dn, True):
                    s.append(pltpu.make_async_copy(mvout.at[b, 2 * half + k, pl.ds(at_, size)], view, mvout_sem.at[b, 2 * half + k]))
        return s

    def moment_stores_wait(kind, p):
        b, rows = lax.rem(p, 2), pl.ds(0, height(kind))
        for k in range(4):
            pltpu.make_async_copy(mvout.at[b, k, rows], mvout.at[b, k, rows], mvout_sem.at[b, k]).wait()

    def own_copies(kind, p):
        s = lax.rem(p, RING)
        return [
            pltpu.make_async_copy(wnew.at[s, half, pl.ds(at_, size)], view, loc_sem.at[half, s])
            for half in range(2)
            for view, at_, size in new_pieces(kind, p, me, half)
        ]

    def kept_copies(kind, p):
        s, h = lax.rem(p, RING), height(kind)
        return [
            pltpu.make_async_copy(wnew.at[s, half, pl.ds(0, h)], (kept_a, kept_b)[half].at[kept_rows(kind, p)], loc_sem.at[half, s]) for half in range(2)
        ]

    def leaves(p):
        return p < packs - KEPT

    def stage(kind, p):
        s, h = lax.rem(p, RING), height(kind)
        if kind == GU:
            def part(dev, half):
                return accgu[pl.ds(mult(dev * q, q), q), half * q : (half + 1) * q].astype(BF16)
        else:
            slot = lax.rem(down_group(p), 2)

            def part(dev, half):
                return dbuf[slot, pl.ds(mult(dev * (2 * h) + half * h, UNIT // 2), h), pl.ds(down_cols(p), q)]
        send[s, 0, :h, :] = part(far, 0)
        send[s, 0, h : 2 * h, :] = part(right, 1)
        send[s, 1, :h, :] = part(far, 1)
        send[s, 1, h : 2 * h, :] = part(left, 0)
        keep[s, 0, :h, :] = part(right, 0)
        keep[s, 1, :h, :] = part(left, 1)
        own[s, 0, :h, :] = part(me, 0)
        own[s, 1, :h, :] = part(me, 1)

    def do_s1(kind, p):
        stage(kind, p)
        for way in range(2):
            s1_copy(kind, p, way).start()

    def do_s2(kind, p):
        s, h = lax.rem(p, RING), height(kind)
        for c in moment_loads(kind, p):
            c.start()
        for way in range(2):
            s1_copy(kind, p, way).wait_recv()
            s2[s, way, :h, :] = (keep[s, way, :h, :].astype(F32) + r1[s, way, :h, :].astype(F32)).astype(BF16)
            s2_copy(kind, p, way).start()

    def do_s3(kind, p):
        s, b, h = lax.rem(p, RING), lax.rem(p, 2), height(kind)
        moment_loads_wait(kind, p)
        for k, cond in kind_of(p - 2).items():
            @pl.when(cond & (p >= 2))
            def _():
                moment_stores_wait(k, p - 2)
        for way in range(2):
            s2_copy(kind, p, way).wait_recv()

        def rows_of(u, _):
            rows = pl.ds(mult(u * (UNIT // 2), UNIT // 2), UNIT // 2)
            rest = pl.ds(mult(h + u * (UNIT // 2), UNIT // 2), UNIT // 2)
            for half in range(2):
                g = own[s, half, rows, :].astype(F32) + r1[s, 1 - half, rest, :].astype(F32) + r2[s, half, rows, :].astype(F32)
                g = g.astype(BF16).astype(F32)
                w, m, v = adamw(win[b, half, rows, :].astype(F32), mvin[b, 2 * half, rows, :], mvin[b, 2 * half + 1, rows, :], g)
                wnew[s, half, rows, :] = w
                mvout[b, 2 * half, rows, :] = m
                mvout[b, 2 * half + 1, rows, :] = v
            return 0

        lax.fori_loop(0, h // (UNIT // 2), rows_of, 0)
        for c in moment_stores(kind, p):
            c.start()

        @pl.when(leaves(p))
        def _():
            for way in range(2):
                for half in ((0, 1), (1, 0))[way]:
                    for c in g1_copies(kind, p, way, half):
                        c.start()
            for c in own_copies(kind, p):
                c.start()

        @pl.when(jnp.logical_not(leaves(p)))
        def _():
            for c in kept_copies(kind, p):
                c.start()

    def do_s4(kind, p):
        s = lax.rem(p, RING)
        for way in range(2):
            s1_copy(kind, p, way).wait_send()
            s2_copy(kind, p, way).wait_send()

        @pl.when(leaves(p))
        def _():
            for way in range(2):
                for half in ((0, 1), (1, 0))[way]:
                    total_of(kind, p, way, half, (g1s.at[way, half, s], g1r.at[way, half, s]), 1)
                    if half == way:
                        for c in g2_copies(kind, p, way):
                            c.start()

    def do_s5(kind, p):
        s, rows = lax.rem(p, RING), pl.ds(0, height(kind))
        far_s = lax.rem(p, 2 * RING)

        @pl.when(leaves(p))
        def _():
            for way in range(2):
                for half in range(2):
                    total_of(kind, p, way, half, (g1s.at[way, half, s], g1r.at[way, half, s]), 0)
                total_of(kind, p, way, way, (g2s.at[way, far_s], g2r.at[way, far_s]), 1)
                total_of(kind, p, way, way, (g2s.at[way, far_s], g2r.at[way, far_s]), 0)

        for half in range(2):
            pltpu.make_async_copy(wnew.at[s, half, rows], wnew.at[s, half, rows], loc_sem.at[half, s]).wait()

    def each(do, p, among=(GU, DOWN, LAST)):
        for kind, cond in kind_of(p).items():
            if kind in among:
                @pl.when(cond & (p >= 0) & (p < packs))
                def _():
                    do(kind, p)

    deep = LEAD + 1

    def lagged(do, p, first, among=(GU, DOWN, LAST)):
        early = p - first < deep
        each(do, jnp.where(early, p - first, jnp.where(p - first == deep, -1, p - first - 1)), among)

    def full(p, among=(GU, DOWN, LAST)):
        each(do_s1, p, among)
        lagged(do_s3, p, 1)

    def half(p):
        lagged(do_s2, p, 0)
        lagged(do_s4, p, 2)
        each(do_s5, p - 5)


    def weight_loads(it):
        b, lay = lax.rem(it, 2), 1 - it // blocks
        cols = pl.ds(block_cols(it), q)
        return (
            pltpu.make_async_copy(wg_hbm.at[lay, :, cols], wgu.at[b, :, pl.ds(0, q)], weight_sem.at[b, 0]),
            pltpu.make_async_copy(wu_hbm.at[lay, :, cols], wgu.at[b, :, pl.ds(q, q)], weight_sem.at[b, 1]),
            pltpu.make_async_copy(wd_hbm.at[lay, cols, :], wdn.at[b], weight_sem.at[b, 2]),
        )

    def tile_loads(a_hbm, d_hbm, t):
        b, rows = lax.rem(t, 2), pl.ds(mult(t * tm, tm), tm)
        return (
            pltpu.make_async_copy(a_hbm.at[rows, :], tiles.at[b, 0], tile_sem.at[b, 0]),
            pltpu.make_async_copy(d_hbm.at[rows, :], tiles.at[b, 1], tile_sem.at[b, 1]),
        )

    def start_tile(layer_1, t):
        @pl.when(layer_1)
        def _():
            for c in tile_loads(a1_hbm, dy_hbm, t):
                c.start()

        @pl.when(jnp.logical_not(layer_1))
        def _():
            for c in tile_loads(a0_hbm, dh_hbm, t):
                c.start()

    def compute(b, wb, t, layer_1):
        a, dh = tiles[b, 0], tiles[b, 1]
        m = tm // 2
        at[...] = a.T
        dht[...] = dh.T
        dact = [dot(dh[r], wdt[...]) for r in (slice(0, m), slice(m, tm))]
        gu = [dot(a[r], wgu[wb]) for r in (slice(0, m), slice(m, tm))]
        for k in range(2):
            rows = slice(k * m, (k + 1) * m)
            gate, up = gu[k][:, :q], gu[k][:, q:]
            dk = dact[k].astype(BF16).astype(F32)
            s = jax.nn.sigmoid(gate)
            silu = gate * s
            act = (silu * up).astype(BF16)
            dup = (dk * silu).astype(BF16)
            dgate = (dk * up * (s + silu * (1 - s))).astype(BF16)
            dgu = jnp.concatenate([dgate, dup], -1)
            if layer_1:
                da[pl.ds(mult(t * tm + k * m, m), m), :] += dot(dgu, wgut[...])
            accgu[...] += dot(at[:, rows], dgu)
            for r in (slice(0, d // 2), slice(d // 2, d)):
                accd[r, :] += dot(dht[r, rows], act)

    def between_layers():
        def loads(t):
            return tile_loads(h1_hbm, dy_hbm, t)

        def store(t):
            return pltpu.make_async_copy(hout.at[lax.rem(t, 2)], dh_hbm.at[pl.ds(mult(t * tm, tm), tm), :], hout_sem.at[lax.rem(t, 2)])

        for c in loads(0):
            c.start()

        def tile(t, _):
            @pl.when(t + 1 < steps)
            def _():
                for c in loads(t + 1):
                    c.start()

            for c in loads(t):
                c.wait()

            @pl.when(t >= 2)
            def _():
                store(t - 2).wait()

            b = lax.rem(t, 2)
            g = da[pl.ds(mult(t * tm, tm), tm), :].astype(BF16).astype(F32)
            wide = tiles[b, 0].astype(F32)
            scale = norm_scale(wide)
            inner = jnp.mean(g * wide, -1, keepdims=True)
            hout[b] = tiles[b, 1] + (scale * g - wide * (scale * scale * scale * inner)).astype(BF16)
            store(t).start()
            return 0

        lax.fori_loop(0, steps, tile, 0)
        store(steps - 2).wait()
        store(steps - 1).wait()

    for c in weight_loads(0):
        c.start()
    start_tile(True, 0)
    da[...] = jnp.zeros_like(da)

    def block(it, _):
        layer_1 = it < blocks
        wb, i = lax.rem(it, 2), lax.rem(it, blocks)
        p = pack_of_block(it)
        with_down = it >= LEAD

        @pl.when(it == blocks)
        def _():
            between_layers()
            start_tile(False, 0)

        for c in weight_loads(it):
            c.wait()

        @pl.when(it + 1 < 2 * blocks)
        def _():
            for c in weight_loads(it + 1):
                c.start()

        wdt[...] = wdn[wb].T

        @pl.when(layer_1)
        def _():
            wgut[...] = wgu[wb].T

        accgu[...] = jnp.zeros_like(accgu)
        accd[...] = jnp.zeros_like(accd)

        def tile(t, _):
            b = lax.rem(t, 2)
            for c in tile_loads(a1_hbm, dy_hbm, t):
                c.wait()

            more = (t + 1 < steps) | ((it + 1 != blocks) & (it + 1 != 2 * blocks))

            @pl.when(more)
            def _():
                start_tile(layer_1, lax.rem(t + 1, steps))

            @pl.when(layer_1)
            def _():
                compute(b, wb, t, True)

            @pl.when(jnp.logical_not(layer_1))
            def _():
                compute(b, wb, t, False)

            @pl.when((t == 1) & (it >= 1))
            def _():
                half(pack_of_block(it - 1))

            @pl.when((t == 3) & with_down)
            def _():
                full(p - 1, (DOWN, LAST))

            @pl.when((t == 5) & with_down)
            def _():
                half(p - 1)

            return 0

        lax.fori_loop(0, steps, tile, 0)
        k, slot = lax.rem(i, 4), lax.rem(i // 4 + jnp.where(layer_1, 0, 1), 2)
        for c in range(d // q):
            dbuf[slot, pl.ds(mult(k * q, q), q), c * q : (c + 1) * q] = accd[c * q : (c + 1) * q, :].astype(BF16).T
        full(p, (GU,))
        return 0

    lax.fori_loop(0, 2 * blocks, block, 0)
    end = packs

    def tail(p, _):
        half(p)
        full(p + 1, (DOWN, LAST))
        return 0

    lax.fori_loop(4 * blocks - LEAD - 1, end + 5, tail, 0)
    for p in (end - 2, end - 1):
        moment_stores_wait(LAST, p)


def backward(a1, dy, h1, a0, wg, wu, wd, moments, n, axis, tm=None):
    tm = tm or TM
    t, d = dy.shape
    ff = wg.shape[-1]
    q = BLOCK
    V = pltpu.VMEM
    DMA = pltpu.SemaphoreType.DMA
    mg, mu, md, vg, vu, vd = moments
    outs = [jax.ShapeDtypeStruct(w.shape, BF16) for w in (wg, wu, wd)]
    outs += [jax.ShapeDtypeStruct(m.shape, F32) for m in moments]
    outs += [jax.ShapeDtypeStruct((t, d), BF16), *[jax.ShapeDtypeStruct((kept_height(), q), BF16)] * 2]
    return pl.pallas_call(
        functools.partial(backward_kernel, n, t // tm, d, ff, axis),
        in_specs=[ANY] * 13,
        out_specs=[ANY] * 12,
        out_shape=outs,
        scratch_shapes=[
            V((2, 2, tm, d), BF16),
            V((d, tm), BF16),
            V((d, tm), BF16),
            V((2, d, 2 * q), BF16),
            V((2, q, d), BF16),
            V((d, q), BF16),
            V((2 * q, d), BF16),
            V((d, 2 * q), F32),
            V((d, q), F32),
            V((t, d), F32),
            V((2, 4 * q, d), BF16),
            V((2, tm, d), BF16),
            V((RING, 2, 2 * q, q), BF16),
            V((RING, 2, q, q), BF16),
            V((RING, 2, q, q), BF16),
            V((RING, 2, 2 * q, q), BF16),
            V((RING, 2, q, q), BF16),
            V((RING, 2, q, q), BF16),
            V((RING, 2, q, q), BF16),
            V((2, 4, q, q), F32),
            V((2, 2, q, q), BF16),
            V((2, 4, q, q), F32),
            DMA((2, 2)),
            DMA((2, 3)),
            DMA((2,)),
            DMA((2, RING)),
            DMA((2, RING)),
            DMA((2, RING)),
            DMA((2, RING)),
            DMA((2, 2, RING)),
            DMA((2, 2, RING)),
            DMA((2, 2 * RING)),
            DMA((2, 2 * RING)),
            DMA((2, RING)),
            DMA((2, 6)),
            DMA((2, 4)),
        ],
        compiler_params=pltpu.CompilerParams(vmem_limit_bytes=62 * MIB, collective_id=0, has_side_effects=True),
        cost_estimate=pl.CostEstimate(flops=28 * t * d * ff, bytes_accessed=44 * t * d, transcendentals=2 * t * ff),
        name="backward",
    )(a1, dy, h1, a0, wg, wu, wd, *moments)


def kept_height():
    return 3 * BLOCK + 4 * (BLOCK // 2) + 4 * (3 * UNIT // 2)


def results_kernel(count, rows, *refs):
    sources, rest = refs[:count], refs[count + 1 :]
    outs, rest = rest[:count], rest[count:]
    kinds = []
    for r in sources:
        if (key := (r.shape[1:], r.dtype)) not in kinds:
            kinds.append(key)
    buffers, (isem, osem) = rest[: len(kinds)], rest[len(kinds) :]
    steps, used = [], [0] * len(kinds)
    for k, r in enumerate(sources):
        kind = kinds.index((r.shape[1:], r.dtype))
        size = buffers[kind].shape[1]
        for lay in range(r.shape[0]):
            for at_ in range(0, r.shape[1], size):
                steps.append((k, kind, used[kind] % SLOTS, lay, at_, size))
                used[kind] += 1

    def copy_in(step):
        k, kind, slot, lay, at_, size = steps[step]
        return pltpu.make_async_copy(sources[k].at[lay, pl.ds(at_, size)], buffers[kind].at[slot], isem.at[kind, slot])

    def copy_out(step):
        k, kind, slot, lay, at_, size = steps[step]
        return pltpu.make_async_copy(buffers[kind].at[slot], outs[k].at[lay, pl.ds(at_, size)], osem.at[kind, slot])

    flying = {}

    def start_in(step):
        key = steps[step][1:3]
        if key in flying:
            copy_out(flying.pop(key)).wait()
        copy_in(step).start()

    for step in range(min(AHEAD, len(steps))):
        start_in(step)
    for step in range(len(steps)):
        copy_in(step).wait()
        copy_out(step).start()
        flying[steps[step][1:3]] = step
        if step + AHEAD < len(steps):
            start_in(step + AHEAD)
    for step in flying.values():
        copy_out(step).wait()


def results(sources, token):
    piece = 128 * 2816 * 2
    kinds = []
    for r in sources:
        if (key := (r.shape[1:], r.dtype)) not in kinds:
            kinds.append(key)
    buffers = []
    for (_, width), dtype in kinds:
        buffers.append(pltpu.VMEM((SLOTS, piece // (width * dtype.itemsize), width), dtype))
    size = sum(r.size * r.dtype.itemsize for r in sources)
    return pl.pallas_call(
        functools.partial(results_kernel, len(sources), None),
        in_specs=[ANY] * (len(sources) + 1),
        out_specs=[ANY] * len(sources),
        out_shape=[jax.ShapeDtypeStruct(r.shape, r.dtype) for r in sources],
        scratch_shapes=buffers + [pltpu.SemaphoreType.DMA((len(kinds), SLOTS))] * 2,
        compiler_params=pltpu.CompilerParams(vmem_limit_bytes=62 * MIB),
        cost_estimate=pl.CostEstimate(flops=20 * 10**9, bytes_accessed=2 * size, transcendentals=0),
        name="results",
    )(*sources, token)


def kept_kernel(n, axis, blocks, a, b, la, lb, ra, rb, fa, fb, ng, nu, nd, ng_out, nu_out, nd_out, sem):
    q, u = BLOCK, UNIT
    me = lax.axis_index(axis)
    ff = nd_out.shape[1]
    mult = pl.multiple_of
    copies = []

    def put(src, dst):
        copies.append(pltpu.make_async_copy(src, dst, sem.at[len(copies)]))

    def cols(b):
        return pl.ds((3 * (b % 4) + b // 4) * q, q)

    for far, halves in enumerate(((a, b), (ra, rb), (fa, fb), (la, lb))):
        dev = lax.rem(me + far, n)
        base = dev * (ff // n)
        for half, src in enumerate(halves):
            out = (ng_out, nu_out)[half]
            rows = pl.ds(mult(dev * q, q), q)
            pair = q + q // 2
            for k in range(3):
                put(src.at[pl.ds(k * pair, q)], out.at[0, rows, cols(blocks - 3 + k)])
            for quarter, at_ in enumerate((q, pair + q, 2 * pair + q, 3 * pair)):
                row = pl.ds(mult(base + 4 * u + dev * u + half * (q // 2), u), q // 2)
                put(src.at[pl.ds(at_, q // 2)], nd_out.at[0, row, pl.ds(quarter * q, q)])
            for quarter in range(4):
                at_ = 3 * pair + q // 2 + quarter * (3 * u // 2)
                for j in range(3):
                    piece = 3 * half + j
                    v = piece // 2
                    row = base + jnp.where(v < dev, v * u, 8 * u + v * u) + (piece % 2) * (u // 2)
                    put(src.at[pl.ds(at_ + j * (u // 2), u // 2)], nd_out.at[0, pl.ds(mult(row, u // 2), u // 2), pl.ds(quarter * q, q)])
    for c in copies:
        c.start()
    for c in copies:
        c.wait()


def place_kept(own, parts, weights, n, axis):
    blocks = weights[0].shape[-1] // BLOCK
    vmem = pl.BlockSpec(memory_space=pltpu.VMEM)
    return pl.pallas_call(
        functools.partial(kept_kernel, n, axis, blocks),
        in_specs=[vmem] * 8 + [ANY] * 3,
        out_specs=[ANY] * 3,
        out_shape=[jax.ShapeDtypeStruct(w.shape, w.dtype) for w in weights],
        input_output_aliases={8: 0, 9: 1, 10: 2},
        scratch_shapes=[pltpu.SemaphoreType.DMA((8 * (3 + 4 + 12),))],
        compiler_params=pltpu.CompilerParams(vmem_limit_bytes=40 * MIB),
        name="place_kept",
    )(*own, *parts, *weights)


def solution(mesh):
    n = mesh.shape["dp"]
    to_right = [(k, (k + 1) % n) for k in range(n)]
    to_left = [(k, (k - 1) % n) for k in range(n)]

    def step(x, dy, wg, wu, wd, m_g, m_u, m_d, v_g, v_u, v_d):
        x, dy = x[0], dy[0]
        a0, h1, a1 = forward(x, wg, wu, wd)
        *made, _, a, b = backward(a1, dy, h1, a0, wg, wu, wd, (m_g, m_u, m_d, v_g, v_u, v_d), n, "dp")
        with jax.named_scope("first"):
            la, rb = lax.ppermute(a, "dp", to_right), lax.ppermute(b, "dp", to_left)
            lb, ra = lax.ppermute(b, "dp", to_right), lax.ppermute(a, "dp", to_left)
        moments = results(made[3:], a)
        with jax.named_scope("second"):
            fa, fb = lax.ppermute(la, "dp", to_right), lax.ppermute(rb, "dp", to_left)
        weights = results(made[:3], moments[0])
        new = place_kept((a, b), (la, lb, ra, rb, fa, fb), weights, n, "dp")
        return (*new, *moments)

    seq = P(("rep", "dp"), None, None)
    rows = P(None, "dp", None)
    whole = P("rep", None, None)
    part = P("rep", "dp", None)
    return jax.shard_map(
        step,
        mesh=mesh,
        in_specs=(seq, seq, P(), P(), P()) + (rows,) * 6,
        out_specs=(whole,) * 3 + (part,) * 6,
        check_vma=False,
    )
```

```python
import functools

import jax
import jax.numpy as jnp
from jax import lax
from jax.experimental import pallas as pl
from jax.experimental.pallas import tpu as pltpu
from jax.sharding import PartitionSpec as P

F32, BF16 = jnp.float32, jnp.bfloat16
BLOCK = 256
UNIT = 64
MIB = 2**20
TM = 512
ANY = pl.BlockSpec(memory_space=pl.ANY)


def dot(a, b):
    return jnp.dot(a, b, preferred_element_type=F32)


def norm_scale(wide):
    return lax.rsqrt(jnp.mean(wide * wide, -1, keepdims=True) + 1e-6)


def params(limit=60):
    return pltpu.CompilerParams(vmem_limit_bytes=limit * MIB, dimension_semantics=("arbitrary",))


def forward_kernel(blocks, x_ref, wg_hbm, wu_hbm, wd_hbm, a0_ref, h_ref, a1_ref, wg, wu, wd, act, sems):
    step = pl.program_id(0)

    def copies(b):
        cols = pl.ds(b * BLOCK, BLOCK)
        return (
            pltpu.make_async_copy(wg_hbm.at[0, :, cols], wg.at[:, cols], sems.at[0, b]),
            pltpu.make_async_copy(wu_hbm.at[0, :, cols], wu.at[:, cols], sems.at[1, b]),
            pltpu.make_async_copy(wd_hbm.at[0, cols, :], wd.at[cols, :], sems.at[2, b]),
        )

    @pl.when(step == 0)
    def _():
        for b in range(blocks):
            for c in copies(b):
                c.start()

    tm = x_ref.shape[0]
    halves = (slice(0, tm // 2), slice(tm // 2, tm))

    def hidden(rows, cols):
        gate = dot(a0_ref[rows, :], wg[:, cols])
        up = dot(a0_ref[rows, :], wu[:, cols])
        act[rows, cols] = (gate * jax.nn.sigmoid(gate) * up).astype(BF16)

    def norm(rows):
        wide = x_ref[rows, :].astype(F32)
        a0_ref[rows, :] = (wide * norm_scale(wide)).astype(BF16)

    def first():
        norm(slice(0, tm))

        def block(b, _):
            for c in copies(b)[:2]:
                c.wait()
            hidden(slice(0, tm), pl.ds(pl.multiple_of(b * BLOCK, BLOCK), BLOCK))
            return 0

        lax.fori_loop(0, blocks, block, 0)
        for b in range(blocks):
            copies(b)[2].wait()

    def finish(rows):
        h = x_ref[rows, :] + dot(act[rows, :], wd[...]).astype(BF16)
        h_ref[rows, :] = h
        wide = h.astype(F32)
        a1_ref[rows, :] = (wide * norm_scale(wide)).astype(BF16)

    @pl.when(step == 0)
    def _():
        first()
        for rows in halves:
            finish(rows)

    @pl.when(step > 0)
    def _():
        for rows in halves:
            norm(rows)
            for b in range(blocks):
                hidden(rows, slice(b * BLOCK, (b + 1) * BLOCK))
        for rows in halves:
            finish(rows)


def forward(x, wg, wu, wd, tm=None):
    tm = tm or TM
    t, d = x.shape
    ff = wg.shape[-1]
    blocks = ff // BLOCK
    tile = pl.BlockSpec((tm, d), lambda i: (i, 0))
    return pl.pallas_call(
        functools.partial(forward_kernel, blocks),
        grid=(t // tm,),
        in_specs=[tile, ANY, ANY, ANY],
        out_specs=[tile] * 3,
        out_shape=[jax.ShapeDtypeStruct((t, d), BF16)] * 3,
        scratch_shapes=[
            pltpu.VMEM((d, ff), BF16),
            pltpu.VMEM((d, ff), BF16),
            pltpu.VMEM((ff, d), BF16),
            pltpu.VMEM((tm, ff), BF16),
            pltpu.SemaphoreType.DMA((3, blocks)),
        ],
        compiler_params=params(),
        cost_estimate=pl.CostEstimate(flops=6 * t * d * ff, bytes_accessed=8 * t * d + 6 * d * ff, transcendentals=t * ff),
        name="forward",
    )(x, wg, wu, wd)


def adamw(w, m, v, g):
    m = 0.9 * m + 0.1 * g
    v = 0.95 * v + 0.05 * g * g
    step = m * lax.rsqrt(v + 1e-8) + 0.1 * w
    return (w - 0.02 * step).astype(BF16), m, v


GU, DOWN, SMALL = 0, 1, 2
RING = 6
LEAD = 3
QUARTERS = 4
GROUPS = 3
KEPT = 12
SLOTS = 12
AHEAD = 6


def pack_of_block(it):
    return jnp.where(it < LEAD, it, 2 * it - LEAD + 1)


def pairs_end(blocks):
    return 4 * blocks - LEAD


def pack_kind(p, blocks):
    down = ((p >= LEAD) & (p < pairs_end(blocks)) & (lax.rem(p + LEAD, 2) == 0)) | (p >= pairs_end(blocks))
    small = down & (lax.rem(pack_down(p, blocks) // QUARTERS, GROUPS) == 0)
    return {GU: jnp.logical_not(down), DOWN: down & jnp.logical_not(small), SMALL: small}


def pack_block(p):
    return jnp.where(p < LEAD, p, (p + LEAD - 1) // 2)


def pack_down(p, blocks):
    return jnp.where(p < pairs_end(blocks), jnp.maximum(p - LEAD, 0) // 2, p - 2 * blocks)


def block_of(i):
    j = i - LEAD
    if isinstance(i, int):
        return 3 * i + 2 if i < LEAD else 3 * (j % 4) + j // 4
    j = jnp.maximum(j, 0)
    return jnp.where(i < LEAD, 3 * i + 2, 3 * lax.rem(j, 4) + j // 4)


def backward_kernel(
    n, steps, d, ff, axis,
    a1_hbm, dy_hbm, h1_hbm, a0_hbm, wg_hbm, wu_hbm, wd_hbm, mg_hbm, mu_hbm, md_hbm, vg_hbm, vu_hbm, vd_hbm,
    ng_hbm, nu_hbm, nd_hbm, mg_out, mu_out, md_out, vg_out, vu_out, vd_out, dh_hbm, kept_a, kept_b,
    tiles, at, dht, wgu, wdn, wdt, wgut, accgu, accd, da, dbuf, hout,
    send, keep, own, r1, r2, s2, wnew, mvin, win, mvout,
    tile_sem, weight_sem, hout_sem, s1s, s1r, s2s, s2r, g1s, g1r, g2s, g2r, loc_sem, mvin_sem, mvout_sem,
):
    tm = tiles.shape[2]
    blocks = ff // BLOCK
    packs = 2 * blocks + 2 * GROUPS * QUARTERS
    q = BLOCK
    me = lax.axis_index(axis)
    right, left, far = (lax.rem(me + k, n) for k in (1, n - 1, 2))
    to = ({axis: right}, {axis: left})
    mult = pl.multiple_of

    barrier = pltpu.get_barrier_semaphore()
    for dev in to:
        pl.semaphore_signal(barrier, inc=1, device_id=dev, device_id_type=pl.DeviceIdType.MESH)
    pl.semaphore_wait(barrier, 2)


    kind_of = functools.partial(pack_kind, blocks=blocks)

    def block_cols(it):
        return mult(block_of(lax.rem(it, blocks)) * q, q)

    def down_group(p):
        return pack_down(p, blocks) // QUARTERS

    def down_cols(p):
        return mult(lax.rem(pack_down(p, blocks), QUARTERS) * q, q)

    def height(kind):
        return {GU: q, DOWN: q // 2, SMALL: 3 * UNIT // 2}[kind]

    def last_row(dev, k):
        u = k // 2
        return mult(jnp.where(u < dev, u * UNIT, 8 * UNIT + u * UNIT) + (k % 2) * (UNIT // 2), UNIT // 2)

    def rows_in(kind, p, dev, half, ref_gu, ref_d, per_device):
        if kind == GU:
            it = pack_block(p)
            base = 0 if per_device else mult(dev * q, q)
            return [(ref_gu[half].at[1 - it // blocks, pl.ds(base, q), pl.ds(block_cols(it), q)], 0, q)]
        group = down_group(p)
        lay, cols = 1 - group // GROUPS, pl.ds(down_cols(p), q)
        base = 0 if per_device else dev * (ff // n)
        if kind == DOWN:
            row = base + (lax.rem(group, GROUPS) - 1) * 4 * UNIT + dev * UNIT + half * (q // 2)
            return [(ref_d.at[lay, pl.ds(mult(row, UNIT), q // 2), cols], 0, q // 2)]
        small = UNIT // 2
        return [
            (ref_d.at[lay, pl.ds(mult(base + last_row(dev, 3 * half + k), small), small), cols], k * small, small) for k in range(3)
        ]

    def kept_rows(kind, p):
        k = p - (packs - KEPT)
        small = q // 2
        pair = q + small
        if kind == GU:
            row = k // 2 * pair
        else:
            row = jnp.where(k < 8, k // 2 * pair + q, 4 * pair + (k - 8) * small)
        return pl.ds(mult(row, UNIT // 2), height(kind))

    def new_pieces(kind, p, dev, half):
        return rows_in(kind, p, dev, half, (ng_hbm, nu_hbm), nd_hbm, False)


    def s1_copy(kind, p, way):
        s, h = lax.rem(p, RING), height(kind)
        rows = pl.ds(0, 2 * h)
        return pltpu.make_async_remote_copy(
            send.at[s, way, rows], r1.at[s, way, rows], s1s.at[way, s], s1r.at[way, s], to[way], pl.DeviceIdType.MESH
        )

    def s2_copy(kind, p, way):
        s, h = lax.rem(p, RING), height(kind)
        rows = pl.ds(0, h)
        return pltpu.make_async_remote_copy(
            s2.at[s, way, rows], r2.at[s, way, rows], s2s.at[way, s], s2r.at[way, s], to[way], pl.DeviceIdType.MESH
        )

    def g1_copies(kind, p, way, half):
        s = lax.rem(p, RING)
        return [
            pltpu.make_async_remote_copy(
                wnew.at[s, half, pl.ds(at_, size)], view, g1s.at[way, half, s], g1r.at[way, half, s], to[way], pl.DeviceIdType.MESH
            )
            for view, at_, size in new_pieces(kind, p, me, half)
        ]

    def g2_copies(kind, p, way):
        s, dev = lax.rem(p, 2 * RING), (left, right)[way]
        return [
            pltpu.make_async_remote_copy(view, view, g2s.at[way, s], g2r.at[way, s], to[way], pl.DeviceIdType.MESH)
            for view, _, _ in new_pieces(kind, p, dev, way)
        ]

    def total_of(kind, p, way, half, sems, side):
        s, h = lax.rem(p, RING), height(kind)
        ref = wnew.at[s, half, pl.ds(0, h)]
        copy = pltpu.make_async_remote_copy(ref, ref, sems[0], sems[1], to[way], pl.DeviceIdType.MESH)
        copy.wait_send() if side == 0 else copy.wait_recv()

    def moment_loads(kind, p):
        b, s = lax.rem(p, 2), []
        for half in range(2):
            for k, (gu, dn) in enumerate((((mg_hbm, mu_hbm), md_hbm), ((vg_hbm, vu_hbm), vd_hbm))):
                for view, at_, size in rows_in(kind, p, me, half, gu, dn, True):
                    s.append(pltpu.make_async_copy(view, mvin.at[b, 2 * half + k, pl.ds(at_, size)], mvin_sem.at[b, 2 * half + k]))
            for view, at_, size in rows_in(kind, p, me, half, (wg_hbm, wu_hbm), wd_hbm, False):
                s.append(pltpu.make_async_copy(view, win.at[b, half, pl.ds(at_, size)], mvin_sem.at[b, 4 + half]))
        return s

    def moment_loads_wait(kind, p):
        b, rows = lax.rem(p, 2), pl.ds(0, height(kind))
        for k in range(4):
            pltpu.make_async_copy(mvin.at[b, k, rows], mvin.at[b, k, rows], mvin_sem.at[b, k]).wait()
        for half in range(2):
            pltpu.make_async_copy(win.at[b, half, rows], win.at[b, half, rows], mvin_sem.at[b, 4 + half]).wait()

    def moment_stores(kind, p):
        b, s = lax.rem(p, 2), []
        for half in range(2):
            for k, (gu, dn) in enumerate((((mg_out, mu_out), md_out), ((vg_out, vu_out), vd_out))):
                for view, at_, size in rows_in(kind, p, me, half, gu, dn, True):
                    s.append(pltpu.make_async_copy(mvout.at[b, 2 * half + k, pl.ds(at_, size)], view, mvout_sem.at[b, 2 * half + k]))
        return s

    def moment_stores_wait(kind, p):
        b, rows = lax.rem(p, 2), pl.ds(0, height(kind))
        for k in range(4):
            pltpu.make_async_copy(mvout.at[b, k, rows], mvout.at[b, k, rows], mvout_sem.at[b, k]).wait()

    def own_copies(kind, p):
        s = lax.rem(p, RING)
        return [
            pltpu.make_async_copy(wnew.at[s, half, pl.ds(at_, size)], view, loc_sem.at[half, s])
            for half in range(2)
            for view, at_, size in new_pieces(kind, p, me, half)
        ]

    def kept_copies(kind, p):
        s, h = lax.rem(p, RING), height(kind)
        return [
            pltpu.make_async_copy(wnew.at[s, half, pl.ds(0, h)], (kept_a, kept_b)[half].at[kept_rows(kind, p)], loc_sem.at[half, s]) for half in range(2)
        ]

    def leaves(p):
        return p < packs - KEPT

    def stage(kind, p):
        s, h = lax.rem(p, RING), height(kind)
        if kind == GU:
            def part(dev, half):
                return accgu[pl.ds(mult(dev * q, q), q), half * q : (half + 1) * q].astype(BF16)
        else:
            slot = lax.rem(down_group(p), 2)

            def part(dev, half):
                return dbuf[slot, pl.ds(mult(dev * (2 * h) + half * h, UNIT // 2), h), pl.ds(down_cols(p), q)]
        send[s, 0, :h, :] = part(far, 0)
        send[s, 0, h : 2 * h, :] = part(right, 1)
        send[s, 1, :h, :] = part(far, 1)
        send[s, 1, h : 2 * h, :] = part(left, 0)
        keep[s, 0, :h, :] = part(right, 0)
        keep[s, 1, :h, :] = part(left, 1)
        own[s, 0, :h, :] = part(me, 0)
        own[s, 1, :h, :] = part(me, 1)

    def do_s1(kind, p):
        stage(kind, p)
        for way in range(2):
            s1_copy(kind, p, way).start()

    def do_s2(kind, p):
        s, h = lax.rem(p, RING), height(kind)
        for c in moment_loads(kind, p):
            c.start()
        for way in range(2):
            s1_copy(kind, p, way).wait_recv()
            s2[s, way, :h, :] = (keep[s, way, :h, :].astype(F32) + r1[s, way, :h, :].astype(F32)).astype(BF16)
            s2_copy(kind, p, way).start()

    def do_s3(kind, p):
        s, b, h = lax.rem(p, RING), lax.rem(p, 2), height(kind)
        moment_loads_wait(kind, p)
        for k, cond in kind_of(p - 2).items():
            @pl.when(cond & (p >= 2))
            def _():
                moment_stores_wait(k, p - 2)
        for way in range(2):
            s2_copy(kind, p, way).wait_recv()

        def rows_of(u, _):
            rows = pl.ds(mult(u * (UNIT // 2), UNIT // 2), UNIT // 2)
            rest = pl.ds(mult(h + u * (UNIT // 2), UNIT // 2), UNIT // 2)
            for half in range(2):
                g = own[s, half, rows, :].astype(F32) + r1[s, 1 - half, rest, :].astype(F32) + r2[s, half, rows, :].astype(F32)
                g = g.astype(BF16).astype(F32)
                w, m, v = adamw(win[b, half, rows, :].astype(F32), mvin[b, 2 * half, rows, :], mvin[b, 2 * half + 1, rows, :], g)
                wnew[s, half, rows, :] = w
                mvout[b, 2 * half, rows, :] = m
                mvout[b, 2 * half + 1, rows, :] = v
            return 0

        lax.fori_loop(0, h // (UNIT // 2), rows_of, 0)
        for c in moment_stores(kind, p):
            c.start()

        @pl.when(leaves(p))
        def _():
            for way in range(2):
                for half in ((0, 1), (1, 0))[way]:
                    for c in g1_copies(kind, p, way, half):
                        c.start()
            for c in own_copies(kind, p):
                c.start()

        if kind != SMALL:
            @pl.when(jnp.logical_not(leaves(p)))
            def _():
                for c in kept_copies(kind, p):
                    c.start()

    def do_s4(kind, p):
        s = lax.rem(p, RING)
        for way in range(2):
            s1_copy(kind, p, way).wait_send()
            s2_copy(kind, p, way).wait_send()

        @pl.when(leaves(p))
        def _():
            for way in range(2):
                for half in ((0, 1), (1, 0))[way]:
                    total_of(kind, p, way, half, (g1s.at[way, half, s], g1r.at[way, half, s]), 1)
                    if half == way:
                        for c in g2_copies(kind, p, way):
                            c.start()

    def do_s5(kind, p):
        s, rows = lax.rem(p, RING), pl.ds(0, height(kind))
        far_s = lax.rem(p, 2 * RING)

        @pl.when(leaves(p))
        def _():
            for way in range(2):
                for half in range(2):
                    total_of(kind, p, way, half, (g1s.at[way, half, s], g1r.at[way, half, s]), 0)
                total_of(kind, p, way, way, (g2s.at[way, far_s], g2r.at[way, far_s]), 1)
                total_of(kind, p, way, way, (g2s.at[way, far_s], g2r.at[way, far_s]), 0)

        for half in range(2):
            pltpu.make_async_copy(wnew.at[s, half, rows], wnew.at[s, half, rows], loc_sem.at[half, s]).wait()

    def each(do, p, among=(GU, DOWN, SMALL)):
        for kind, cond in kind_of(p).items():
            if kind in among:
                @pl.when(cond & (p >= 0) & (p < packs))
                def _():
                    do(kind, p)

    deep = 0

    def lagged(do, p, lag):
        each(do, jnp.where(p < deep, p, jnp.where(p < deep + lag, -1, p - lag)))

    def full(p, among=(GU, DOWN, SMALL)):
        each(do_s1, p, among)
        lagged(do_s3, p - 1, 2)

    def half(p):
        lagged(do_s2, p, 1)
        lagged(do_s4, p - 2, 2)
        each(do_s5, p - 6)


    def weight_loads(it):
        b, lay = lax.rem(it, 2), 1 - it // blocks
        cols = pl.ds(block_cols(it), q)
        return (
            pltpu.make_async_copy(wg_hbm.at[lay, :, cols], wgu.at[b, :, pl.ds(0, q)], weight_sem.at[b, 0]),
            pltpu.make_async_copy(wu_hbm.at[lay, :, cols], wgu.at[b, :, pl.ds(q, q)], weight_sem.at[b, 1]),
            pltpu.make_async_copy(wd_hbm.at[lay, cols, :], wdn.at[b], weight_sem.at[b, 2]),
        )

    def tile_loads(a_hbm, d_hbm, t):
        b, rows = lax.rem(t, 2), pl.ds(mult(t * tm, tm), tm)
        return (
            pltpu.make_async_copy(a_hbm.at[rows, :], tiles.at[b, 0], tile_sem.at[b, 0]),
            pltpu.make_async_copy(d_hbm.at[rows, :], tiles.at[b, 1], tile_sem.at[b, 1]),
        )

    def start_tile(layer_1, t):
        @pl.when(layer_1)
        def _():
            for c in tile_loads(a1_hbm, dy_hbm, t):
                c.start()

        @pl.when(jnp.logical_not(layer_1))
        def _():
            for c in tile_loads(a0_hbm, dh_hbm, t):
                c.start()

    def compute(b, wb, t, layer_1):
        a, dh = tiles[b, 0], tiles[b, 1]
        m = tm // 2
        at[...] = a.T
        dht[...] = dh.T
        dact = [dot(dh[r], wdt[...]) for r in (slice(0, m), slice(m, tm))]
        gu = [dot(a[r], wgu[wb]) for r in (slice(0, m), slice(m, tm))]
        for k in range(2):
            rows = slice(k * m, (k + 1) * m)
            gate, up = gu[k][:, :q], gu[k][:, q:]
            dk = dact[k].astype(BF16).astype(F32)
            s = jax.nn.sigmoid(gate)
            silu = gate * s
            act = (silu * up).astype(BF16)
            dup = (dk * silu).astype(BF16)
            dgate = (dk * up * (s + silu * (1 - s))).astype(BF16)
            dgu = jnp.concatenate([dgate, dup], -1)
            if layer_1:
                da[pl.ds(mult(t * tm + k * m, m), m), :] += dot(dgu, wgut[...])
            accgu[...] += dot(at[:, rows], dgu)
            for r in (slice(0, d // 2), slice(d // 2, d)):
                accd[r, :] += dot(dht[r, rows], act)

    def between_layers():
        def loads(t):
            return tile_loads(h1_hbm, dy_hbm, t)

        def store(t):
            return pltpu.make_async_copy(hout.at[lax.rem(t, 2)], dh_hbm.at[pl.ds(mult(t * tm, tm), tm), :], hout_sem.at[lax.rem(t, 2)])

        for c in loads(0):
            c.start()

        def tile(t, _):
            @pl.when(t + 1 < steps)
            def _():
                for c in loads(t + 1):
                    c.start()

            for c in loads(t):
                c.wait()

            @pl.when(t >= 2)
            def _():
                store(t - 2).wait()

            b = lax.rem(t, 2)
            g = da[pl.ds(mult(t * tm, tm), tm), :].astype(BF16).astype(F32)
            wide = tiles[b, 0].astype(F32)
            scale = norm_scale(wide)
            inner = jnp.mean(g * wide, -1, keepdims=True)
            hout[b] = tiles[b, 1] + (scale * g - wide * (scale * scale * scale * inner)).astype(BF16)
            store(t).start()
            return 0

        lax.fori_loop(0, steps, tile, 0)
        store(steps - 2).wait()
        store(steps - 1).wait()

    for c in weight_loads(0):
        c.start()
    start_tile(True, 0)
    da[...] = jnp.zeros_like(da)

    def block(it, _):
        layer_1 = it < blocks
        wb, i = lax.rem(it, 2), lax.rem(it, blocks)
        p = pack_of_block(it)
        with_down = it >= LEAD

        @pl.when(it == blocks)
        def _():
            between_layers()
            start_tile(False, 0)

        for c in weight_loads(it):
            c.wait()

        @pl.when(it + 1 < 2 * blocks)
        def _():
            for c in weight_loads(it + 1):
                c.start()

        wdt[...] = wdn[wb].T

        @pl.when(layer_1)
        def _():
            wgut[...] = wgu[wb].T

        accgu[...] = jnp.zeros_like(accgu)
        accd[...] = jnp.zeros_like(accd)

        def tile(t, _):
            b = lax.rem(t, 2)
            for c in tile_loads(a1_hbm, dy_hbm, t):
                c.wait()

            more = (t + 1 < steps) | ((it + 1 != blocks) & (it + 1 != 2 * blocks))

            @pl.when(more)
            def _():
                start_tile(layer_1, lax.rem(t + 1, steps))

            @pl.when(layer_1)
            def _():
                compute(b, wb, t, True)

            @pl.when(jnp.logical_not(layer_1))
            def _():
                compute(b, wb, t, False)

            @pl.when((t == 1) & (it >= 1))
            def _():
                half(pack_of_block(it - 1))

            @pl.when((t == 3) & with_down)
            def _():
                full(p - 1, (DOWN, SMALL))

            @pl.when((t == 5) & with_down)
            def _():
                half(p - 1)

            return 0

        lax.fori_loop(0, steps, tile, 0)
        k = jnp.where(i < LEAD, i, lax.rem(jnp.maximum(i - LEAD, 0), 4))
        slot = lax.rem(jnp.where(i < LEAD, 0, (i + 1) // 4) + jnp.where(layer_1, 0, GROUPS), 2)
        for c in range(d // q):
            dbuf[slot, pl.ds(mult(k * q, q), q), c * q : (c + 1) * q] = accd[c * q : (c + 1) * q, :].astype(BF16).T
        full(p, (GU,))
        return 0

    lax.fori_loop(0, 2 * blocks, block, 0)
    end = packs

    def tail(p, _):
        half(p)
        full(p + 1, (DOWN, SMALL))
        return 0

    lax.fori_loop(pairs_end(blocks) - 1, end + 6, tail, 0)
    for p in (end - 2, end - 1):
        moment_stores_wait(DOWN, p)


def backward(a1, dy, h1, a0, wg, wu, wd, moments, n, axis, tm=None):
    tm = tm or TM
    t, d = dy.shape
    ff = wg.shape[-1]
    q = BLOCK
    V = pltpu.VMEM
    DMA = pltpu.SemaphoreType.DMA
    mg, mu, md, vg, vu, vd = moments
    outs = [jax.ShapeDtypeStruct(w.shape, BF16) for w in (wg, wu, wd)]
    outs += [jax.ShapeDtypeStruct(m.shape, F32) for m in moments]
    outs += [jax.ShapeDtypeStruct((t, d), BF16), *[jax.ShapeDtypeStruct((kept_height(), q), BF16)] * 2]
    return pl.pallas_call(
        functools.partial(backward_kernel, n, t // tm, d, ff, axis),
        in_specs=[ANY] * 13,
        out_specs=[ANY] * 12,
        out_shape=outs,
        scratch_shapes=[
            V((2, 2, tm, d), BF16),
            V((d, tm), BF16),
            V((d, tm), BF16),
            V((2, d, 2 * q), BF16),
            V((2, q, d), BF16),
            V((d, q), BF16),
            V((2 * q, d), BF16),
            V((d, 2 * q), F32),
            V((d, q), F32),
            V((t, d), F32),
            V((2, 4 * q, d), BF16),
            V((2, tm, d), BF16),
            V((RING, 2, 2 * q, q), BF16),
            V((RING, 2, q, q), BF16),
            V((RING, 2, q, q), BF16),
            V((RING, 2, 2 * q, q), BF16),
            V((RING, 2, q, q), BF16),
            V((RING, 2, q, q), BF16),
            V((RING, 2, q, q), BF16),
            V((2, 4, q, q), F32),
            V((2, 2, q, q), BF16),
            V((2, 4, q, q), F32),
            DMA((2, 2)),
            DMA((2, 3)),
            DMA((2,)),
            DMA((2, RING)),
            DMA((2, RING)),
            DMA((2, RING)),
            DMA((2, RING)),
            DMA((2, 2, RING)),
            DMA((2, 2, RING)),
            DMA((2, 2 * RING)),
            DMA((2, 2 * RING)),
            DMA((2, RING)),
            DMA((2, 6)),
            DMA((2, 4)),
        ],
        compiler_params=pltpu.CompilerParams(vmem_limit_bytes=62 * MIB, collective_id=0, has_side_effects=True),
        cost_estimate=pl.CostEstimate(flops=28 * t * d * ff, bytes_accessed=44 * t * d, transcendentals=2 * t * ff),
        name="backward",
    )(a1, dy, h1, a0, wg, wu, wd, *moments)


def kept_height():
    return 4 * BLOCK + 8 * (BLOCK // 2)


def results_kernel(count, rows, *refs):
    sources, rest = refs[:count], refs[count + 1 :]
    outs, rest = rest[:count], rest[count:]
    kinds = []
    for r in sources:
        if (key := (r.shape[1:], r.dtype)) not in kinds:
            kinds.append(key)
    buffers, (isem, osem) = rest[: len(kinds)], rest[len(kinds) :]
    steps, used = [], [0] * len(kinds)
    for k, r in enumerate(sources):
        kind = kinds.index((r.shape[1:], r.dtype))
        size = buffers[kind].shape[1]
        for lay in range(r.shape[0]):
            for at_ in range(0, r.shape[1], size):
                steps.append((k, kind, used[kind] % SLOTS, lay, at_, size))
                used[kind] += 1

    def copy_in(step):
        k, kind, slot, lay, at_, size = steps[step]
        return pltpu.make_async_copy(sources[k].at[lay, pl.ds(at_, size)], buffers[kind].at[slot], isem.at[kind, slot])

    def copy_out(step):
        k, kind, slot, lay, at_, size = steps[step]
        return pltpu.make_async_copy(buffers[kind].at[slot], outs[k].at[lay, pl.ds(at_, size)], osem.at[kind, slot])

    flying = {}

    def start_in(step):
        key = steps[step][1:3]
        if key in flying:
            copy_out(flying.pop(key)).wait()
        copy_in(step).start()

    for step in range(min(AHEAD, len(steps))):
        start_in(step)
    for step in range(len(steps)):
        copy_in(step).wait()
        copy_out(step).start()
        flying[steps[step][1:3]] = step
        if step + AHEAD < len(steps):
            start_in(step + AHEAD)
    for step in flying.values():
        copy_out(step).wait()


def results(sources, token):
    piece = 128 * 2816 * 2
    kinds = []
    for r in sources:
        if (key := (r.shape[1:], r.dtype)) not in kinds:
            kinds.append(key)
    buffers = []
    for (_, width), dtype in kinds:
        buffers.append(pltpu.VMEM((SLOTS, piece // (width * dtype.itemsize), width), dtype))
    size = sum(r.size * r.dtype.itemsize for r in sources)
    return pl.pallas_call(
        functools.partial(results_kernel, len(sources), None),
        in_specs=[ANY] * (len(sources) + 1),
        out_specs=[ANY] * len(sources),
        out_shape=[jax.ShapeDtypeStruct(r.shape, r.dtype) for r in sources],
        scratch_shapes=buffers + [pltpu.SemaphoreType.DMA((len(kinds), SLOTS))] * 2,
        compiler_params=pltpu.CompilerParams(vmem_limit_bytes=62 * MIB),
        cost_estimate=pl.CostEstimate(flops=20 * 10**9, bytes_accessed=2 * size, transcendentals=0),
        name="results",
    )(*sources, token)


def kept_kernel(n, axis, blocks, away, *refs):
    halves, (ng_out, nu_out, nd_out, sem) = refs[: 2 * len(away)], refs[2 * len(away) + 3 :]
    q, u = BLOCK, UNIT
    small = q // 2
    pair = q + small
    me = lax.axis_index(axis)
    ff = nd_out.shape[1]
    mult = pl.multiple_of
    copies = []

    def put(src, dst):
        copies.append(pltpu.make_async_copy(src, dst, sem.at[len(copies)]))

    for k, src in enumerate(halves):
        dev, half = lax.rem(me + away[k // 2], n), k % 2
        base = dev * (ff // n)
        out = (ng_out, nu_out)[half]
        rows = pl.ds(mult(dev * q, q), q)
        for b in range(4):
            put(src.at[pl.ds(b * pair, q)], out.at[0, rows, pl.ds(block_of(blocks - 4 + b) * q, q)])
        for b in range(8):
            at_ = b * pair + q if b < 4 else 4 * pair + (b - 4) * small
            row = pl.ds(mult(base + b // 4 * 4 * u + dev * u + half * small, u), small)
            put(src.at[pl.ds(at_, small)], nd_out.at[0, row, pl.ds(b % 4 * q, q)])
    for c in copies:
        c.start()
    for c in copies:
        c.wait()


def place_kept(parts, away, weights, n, axis):
    blocks = weights[0].shape[-1] // BLOCK
    vmem = pl.BlockSpec(memory_space=pltpu.VMEM)
    count = len(parts)
    return pl.pallas_call(
        functools.partial(kept_kernel, n, axis, blocks, away),
        in_specs=[vmem] * count + [ANY] * 3,
        out_specs=[ANY] * 3,
        out_shape=[jax.ShapeDtypeStruct(w.shape, w.dtype) for w in weights],
        input_output_aliases={count + k: k for k in range(3)},
        scratch_shapes=[pltpu.SemaphoreType.DMA((count * 12,))],
        compiler_params=pltpu.CompilerParams(vmem_limit_bytes=62 * MIB),
        cost_estimate=pl.CostEstimate(flops=10**9, bytes_accessed=count * 4 * MIB, transcendentals=0),
        name="place_kept",
    )(*parts, *weights)


def solution(mesh):
    n = mesh.shape["dp"]
    to_right = [(k, (k + 1) % n) for k in range(n)]
    to_left = [(k, (k - 1) % n) for k in range(n)]

    def step(x, dy, wg, wu, wd, m_g, m_u, m_d, v_g, v_u, v_d):
        x, dy = x[0], dy[0]
        a0, h1, a1 = forward(x, wg, wu, wd)
        ng, nu, nd, mg, mu, md, vg, vu, vd, _, a, b = backward(a1, dy, h1, a0, wg, wu, wd, (m_g, m_u, m_d, v_g, v_u, v_d), n, "dp")
        la, rb = lax.ppermute(a, "dp", to_right), lax.ppermute(b, "dp", to_left)
        mg, mu, vg, vu = results((mg, mu, vg, vu), a)
        a, b, mg = lax.optimization_barrier((a, b, mg))
        lb, ra = lax.ppermute(b, "dp", to_right), lax.ppermute(a, "dp", to_left)
        md, vd, nd = results((md, vd, nd), mg)
        la, rb, md = lax.optimization_barrier((la, rb, md))
        fa, fb = lax.ppermute(la, "dp", to_right), lax.ppermute(rb, "dp", to_left)
        ng, nu = results((ng, nu), md)
        new = place_kept((a, b, ra, rb, la, lb), (0, 1, n - 1), (ng, nu, nd), n, "dp")
        new = place_kept((fa, fb), (2,), new, n, "dp")
        return (*new, mg, mu, md, vg, vu, vd)

    seq = P(("rep", "dp"), None, None)
    rows = P(None, "dp", None)
    whole = P("rep", None, None)
    part = P("rep", "dp", None)
    return jax.shard_map(
        step,
        mesh=mesh,
        in_specs=(seq, seq, P(), P(), P()) + (rows,) * 6,
        out_specs=(whole,) * 3 + (part,) * 6,
        check_vma=False,
    )
```

```python
import functools

import jax
import jax.numpy as jnp
from jax import lax
from jax.experimental import pallas as pl
from jax.experimental.pallas import tpu as pltpu
from jax.sharding import PartitionSpec as P

F32, BF16 = jnp.float32, jnp.bfloat16
BLOCK = 256
UNIT = 64
MIB = 2**20
TM = 512
TB = 1024
ANY = pl.BlockSpec(memory_space=pl.ANY)


def dot(a, b):
    return jnp.dot(a, b, preferred_element_type=F32)


def norm_scale(wide):
    return lax.rsqrt(jnp.mean(wide * wide, -1, keepdims=True) + 1e-6)


def params(limit=60):
    return pltpu.CompilerParams(vmem_limit_bytes=limit * MIB, dimension_semantics=("arbitrary",))


def forward_kernel(blocks, x_ref, wg_hbm, wu_hbm, wd_hbm, a0_ref, h_ref, a1_ref, wg, wu, wd, act, sems):
    step = pl.program_id(0)

    def copies(b):
        cols = pl.ds(b * BLOCK, BLOCK)
        return (
            pltpu.make_async_copy(wg_hbm.at[0, :, cols], wg.at[:, cols], sems.at[0, b]),
            pltpu.make_async_copy(wu_hbm.at[0, :, cols], wu.at[:, cols], sems.at[1, b]),
            pltpu.make_async_copy(wd_hbm.at[0, cols, :], wd.at[cols, :], sems.at[2, b]),
        )

    @pl.when(step == 0)
    def _():
        for b in range(blocks):
            for c in copies(b):
                c.start()

    tm = x_ref.shape[0]
    halves = (slice(0, tm // 2), slice(tm // 2, tm))

    def hidden(rows, cols):
        gate = dot(a0_ref[rows, :], wg[:, cols])
        up = dot(a0_ref[rows, :], wu[:, cols])
        act[rows, cols] = (gate * jax.nn.sigmoid(gate) * up).astype(BF16)

    def norm(rows):
        wide = x_ref[rows, :].astype(F32)
        a0_ref[rows, :] = (wide * norm_scale(wide)).astype(BF16)

    def first():
        norm(slice(0, tm))

        def block(b, _):
            for c in copies(b)[:2]:
                c.wait()
            hidden(slice(0, tm), pl.ds(pl.multiple_of(b * BLOCK, BLOCK), BLOCK))
            return 0

        lax.fori_loop(0, blocks, block, 0)
        for b in range(blocks):
            copies(b)[2].wait()

    def finish(rows):
        h = x_ref[rows, :] + dot(act[rows, :], wd[...]).astype(BF16)
        h_ref[rows, :] = h
        wide = h.astype(F32)
        a1_ref[rows, :] = (wide * norm_scale(wide)).astype(BF16)

    @pl.when(step == 0)
    def _():
        first()
        for rows in halves:
            finish(rows)

    @pl.when(step > 0)
    def _():
        for rows in halves:
            norm(rows)
            for b in range(blocks):
                hidden(rows, slice(b * BLOCK, (b + 1) * BLOCK))
        for rows in halves:
            finish(rows)


def forward(x, wg, wu, wd, tm=None):
    tm = tm or TM
    t, d = x.shape
    ff = wg.shape[-1]
    blocks = ff // BLOCK
    tile = pl.BlockSpec((tm, d), lambda i: (i, 0))
    return pl.pallas_call(
        functools.partial(forward_kernel, blocks),
        grid=(t // tm,),
        in_specs=[tile, ANY, ANY, ANY],
        out_specs=[tile] * 3,
        out_shape=[jax.ShapeDtypeStruct((t, d), BF16)] * 3,
        scratch_shapes=[
            pltpu.VMEM((d, ff), BF16),
            pltpu.VMEM((d, ff), BF16),
            pltpu.VMEM((ff, d), BF16),
            pltpu.VMEM((tm, ff), BF16),
            pltpu.SemaphoreType.DMA((3, blocks)),
        ],
        compiler_params=params(),
        cost_estimate=pl.CostEstimate(flops=6 * t * d * ff, bytes_accessed=8 * t * d + 6 * d * ff, transcendentals=t * ff),
        name="forward",
    )(x, wg, wu, wd)


def adamw(w, m, v, g):
    m = 0.9 * m + 0.1 * g
    v = 0.95 * v + 0.05 * g * g
    step = m * lax.rsqrt(v + 1e-8) + 0.1 * w
    return (w - 0.02 * step).astype(BF16), m, v


GU, DOWN, SMALL = 0, 1, 2
RING = 6
KEEP_RING = 3
OWN_RING = 4
LEAD = 3
QUARTERS = 4
GROUPS = 3
KEPT = 12
SLOTS = 12
AHEAD = 6


def pack_of_block(it):
    return jnp.where(it < LEAD, it, 2 * it - LEAD + 1)


def pairs_end(blocks):
    return 4 * blocks - LEAD


def pack_kind(p, blocks):
    down = ((p >= LEAD) & (p < pairs_end(blocks)) & (lax.rem(p + LEAD, 2) == 0)) | (p >= pairs_end(blocks))
    small = down & (lax.rem(pack_down(p, blocks) // QUARTERS, GROUPS) == 0)
    return {GU: jnp.logical_not(down), DOWN: down & jnp.logical_not(small), SMALL: small}


def pack_block(p):
    return jnp.where(p < LEAD, p, (p + LEAD - 1) // 2)


def pack_down(p, blocks):
    return jnp.where(p < pairs_end(blocks), jnp.maximum(p - LEAD, 0) // 2, p - 2 * blocks)


def block_of(i):
    j = i - LEAD
    if isinstance(i, int):
        return 3 * i + 2 if i < LEAD else 3 * (j % 4) + j // 4
    j = jnp.maximum(j, 0)
    return jnp.where(i < LEAD, 3 * i + 2, 3 * lax.rem(j, 4) + j // 4)


def backward_kernel(
    n, steps, d, ff, axis,
    a1_hbm, dy_hbm, h1_hbm, a0_hbm, wg_hbm, wu_hbm, wd_hbm, mg_hbm, mu_hbm, md_hbm, vg_hbm, vu_hbm, vd_hbm,
    ng_hbm, nu_hbm, nd_hbm, mg_out, mu_out, md_out, vg_out, vu_out, vd_out, dh_hbm, kept_a, kept_b,
    tiles, at, dht, wgu, wdn, wdt, wgut, accgu, accd, da, dbuf,
    send, keep, own, r1, r2, s2, wnew, mvin, win, mvout,
    tile_sem, weight_sem, hout_sem, s1s, s1r, s2s, s2r, g1s, g1r, g2s, g2r, loc_sem, mvin_sem, mvout_sem,
):
    tm = tiles.shape[2]
    blocks = ff // BLOCK
    packs = 2 * blocks + 2 * GROUPS * QUARTERS
    q = BLOCK
    me = lax.axis_index(axis)
    right, left, far = (lax.rem(me + k, n) for k in (1, n - 1, 2))
    to = ({axis: right}, {axis: left})
    mult = pl.multiple_of

    barrier = pltpu.get_barrier_semaphore()
    for dev in to:
        pl.semaphore_signal(barrier, inc=1, device_id=dev, device_id_type=pl.DeviceIdType.MESH)
    pl.semaphore_wait(barrier, 2)


    kind_of = functools.partial(pack_kind, blocks=blocks)

    def block_cols(it):
        return mult(block_of(lax.rem(it, blocks)) * q, q)

    def down_group(p):
        return pack_down(p, blocks) // QUARTERS

    def down_cols(p):
        return mult(lax.rem(pack_down(p, blocks), QUARTERS) * q, q)

    def height(kind):
        return {GU: q, DOWN: q // 2, SMALL: 3 * UNIT // 2}[kind]

    def last_row(dev, k):
        u = k // 2
        return mult(jnp.where(u < dev, u * UNIT, 8 * UNIT + u * UNIT) + (k % 2) * (UNIT // 2), UNIT // 2)

    def rows_in(kind, p, dev, half, ref_gu, ref_d, per_device):
        if kind == GU:
            it = pack_block(p)
            base = 0 if per_device else mult(dev * q, q)
            return [(ref_gu[half].at[1 - it // blocks, pl.ds(base, q), pl.ds(block_cols(it), q)], 0, q)]
        group = down_group(p)
        lay, cols = 1 - group // GROUPS, pl.ds(down_cols(p), q)
        base = 0 if per_device else dev * (ff // n)
        if kind == DOWN:
            row = base + (lax.rem(group, GROUPS) - 1) * 4 * UNIT + dev * UNIT + half * (q // 2)
            return [(ref_d.at[lay, pl.ds(mult(row, UNIT), q // 2), cols], 0, q // 2)]
        small = UNIT // 2
        return [
            (ref_d.at[lay, pl.ds(mult(base + last_row(dev, 3 * half + k), small), small), cols], k * small, small) for k in range(3)
        ]

    def kept_rows(kind, p):
        k = p - (packs - KEPT)
        small = q // 2
        pair = q + small
        if kind == GU:
            row = k // 2 * pair
        else:
            row = jnp.where(k < 8, k // 2 * pair + q, 4 * pair + (k - 8) * small)
        return pl.ds(mult(row, UNIT // 2), height(kind))

    def new_pieces(kind, p, dev, half):
        return rows_in(kind, p, dev, half, (ng_hbm, nu_hbm), nd_hbm, False)


    def s1_copy(kind, p, way):
        s, h = lax.rem(p, RING), height(kind)
        rows = pl.ds(0, 2 * h)
        return pltpu.make_async_remote_copy(
            send.at[s, way, rows], r1.at[s, way, rows], s1s.at[way, s], s1r.at[way, s], to[way], pl.DeviceIdType.MESH
        )

    def s2_copy(kind, p, way):
        s, h = lax.rem(p, RING), height(kind)
        rows = pl.ds(0, h)
        return pltpu.make_async_remote_copy(
            s2.at[s, way, rows], r2.at[s, way, rows], s2s.at[way, s], s2r.at[way, s], to[way], pl.DeviceIdType.MESH
        )

    def g1_copies(kind, p, way, half):
        s = lax.rem(p, RING)
        return [
            pltpu.make_async_remote_copy(
                wnew.at[s, half, pl.ds(at_, size)], view, g1s.at[way, half, s], g1r.at[way, half, s], to[way], pl.DeviceIdType.MESH
            )
            for view, at_, size in new_pieces(kind, p, me, half)
        ]

    def g2_copies(kind, p, way):
        s, dev = lax.rem(p, 2 * RING), (left, right)[way]
        return [
            pltpu.make_async_remote_copy(view, view, g2s.at[way, s], g2r.at[way, s], to[way], pl.DeviceIdType.MESH)
            for view, _, _ in new_pieces(kind, p, dev, way)
        ]

    def total_of(kind, p, way, half, sems, side):
        s, h = lax.rem(p, RING), height(kind)
        ref = wnew.at[s, half, pl.ds(0, h)]
        copy = pltpu.make_async_remote_copy(ref, ref, sems[0], sems[1], to[way], pl.DeviceIdType.MESH)
        copy.wait_send() if side == 0 else copy.wait_recv()

    def moment_loads(kind, p):
        b, s = lax.rem(p, 2), []
        for half in range(2):
            for k, (gu, dn) in enumerate((((mg_hbm, mu_hbm), md_hbm), ((vg_hbm, vu_hbm), vd_hbm))):
                for view, at_, size in rows_in(kind, p, me, half, gu, dn, True):
                    s.append(pltpu.make_async_copy(view, mvin.at[b, 2 * half + k, pl.ds(at_, size)], mvin_sem.at[b, 2 * half + k]))
            for view, at_, size in rows_in(kind, p, me, half, (wg_hbm, wu_hbm), wd_hbm, False):
                s.append(pltpu.make_async_copy(view, win.at[b, half, pl.ds(at_, size)], mvin_sem.at[b, 4 + half]))
        return s

    def moment_loads_wait(kind, p):
        b, rows = lax.rem(p, 2), pl.ds(0, height(kind))
        for k in range(4):
            pltpu.make_async_copy(mvin.at[b, k, rows], mvin.at[b, k, rows], mvin_sem.at[b, k]).wait()
        for half in range(2):
            pltpu.make_async_copy(win.at[b, half, rows], win.at[b, half, rows], mvin_sem.at[b, 4 + half]).wait()

    def moment_stores(kind, p):
        b, s = lax.rem(p, 2), []
        for half in range(2):
            for k, (gu, dn) in enumerate((((mg_out, mu_out), md_out), ((vg_out, vu_out), vd_out))):
                for view, at_, size in rows_in(kind, p, me, half, gu, dn, True):
                    s.append(pltpu.make_async_copy(mvout.at[b, 2 * half + k, pl.ds(at_, size)], view, mvout_sem.at[b, 2 * half + k]))
        return s

    def moment_stores_wait(kind, p):
        b, rows = lax.rem(p, 2), pl.ds(0, height(kind))
        for k in range(4):
            pltpu.make_async_copy(mvout.at[b, k, rows], mvout.at[b, k, rows], mvout_sem.at[b, k]).wait()

    def own_copies(kind, p):
        s = lax.rem(p, RING)
        return [
            pltpu.make_async_copy(wnew.at[s, half, pl.ds(at_, size)], view, loc_sem.at[half, s])
            for half in range(2)
            for view, at_, size in new_pieces(kind, p, me, half)
        ]

    def kept_copies(kind, p):
        s, h = lax.rem(p, RING), height(kind)
        return [
            pltpu.make_async_copy(wnew.at[s, half, pl.ds(0, h)], (kept_a, kept_b)[half].at[kept_rows(kind, p)], loc_sem.at[half, s]) for half in range(2)
        ]

    def leaves(p):
        return p < packs - KEPT

    def stage(kind, p):
        s, h = lax.rem(p, RING), height(kind)
        if kind == GU:
            def part(dev, half):
                return accgu[pl.ds(mult(dev * q, q), q), half * q : (half + 1) * q].astype(BF16)
        else:
            slot = lax.rem(down_group(p), 2)

            def part(dev, half):
                return dbuf[slot, pl.ds(mult(dev * (2 * h) + half * h, UNIT // 2), h), pl.ds(down_cols(p), q)]
        send[s, 0, :h, :] = part(far, 0)
        send[s, 0, h : 2 * h, :] = part(right, 1)
        send[s, 1, :h, :] = part(far, 1)
        send[s, 1, h : 2 * h, :] = part(left, 0)
        sk, so = lax.rem(p, KEEP_RING), lax.rem(p, OWN_RING)
        keep[sk, 0, :h, :] = part(right, 0)
        keep[sk, 1, :h, :] = part(left, 1)
        own[so, 0, :h, :] = part(me, 0)
        own[so, 1, :h, :] = part(me, 1)

    def do_s1(kind, p):
        stage(kind, p)
        for way in range(2):
            s1_copy(kind, p, way).start()

    def do_s2(kind, p):
        s, h = lax.rem(p, RING), height(kind)
        for c in moment_loads(kind, p):
            c.start()
        for way in range(2):
            s1_copy(kind, p, way).wait_recv()
            s2[s, way, :h, :] = (keep[lax.rem(p, KEEP_RING), way, :h, :].astype(F32) + r1[s, way, :h, :].astype(F32)).astype(BF16)
            s2_copy(kind, p, way).start()

    def do_s3(kind, p):
        s, b, h = lax.rem(p, RING), lax.rem(p, 2), height(kind)
        moment_loads_wait(kind, p)
        for k, cond in kind_of(p - 2).items():
            @pl.when(cond & (p >= 2))
            def _():
                moment_stores_wait(k, p - 2)
        for way in range(2):
            s2_copy(kind, p, way).wait_recv()

        def rows_of(u, _):
            rows = pl.ds(mult(u * (UNIT // 2), UNIT // 2), UNIT // 2)
            rest = pl.ds(mult(h + u * (UNIT // 2), UNIT // 2), UNIT // 2)
            for half in range(2):
                g = own[lax.rem(p, OWN_RING), half, rows, :].astype(F32) + r1[s, 1 - half, rest, :].astype(F32) + r2[s, half, rows, :].astype(F32)
                g = g.astype(BF16).astype(F32)
                w, m, v = adamw(win[b, half, rows, :].astype(F32), mvin[b, 2 * half, rows, :], mvin[b, 2 * half + 1, rows, :], g)
                wnew[s, half, rows, :] = w
                mvout[b, 2 * half, rows, :] = m
                mvout[b, 2 * half + 1, rows, :] = v
            return 0

        lax.fori_loop(0, h // (UNIT // 2), rows_of, 0)
        for c in moment_stores(kind, p):
            c.start()

        @pl.when(leaves(p))
        def _():
            for way in range(2):
                for half in ((0, 1), (1, 0))[way]:
                    for c in g1_copies(kind, p, way, half):
                        c.start()
            for c in own_copies(kind, p):
                c.start()

        if kind != SMALL:
            @pl.when(jnp.logical_not(leaves(p)))
            def _():
                for c in kept_copies(kind, p):
                    c.start()

    def do_s4(kind, p):
        s = lax.rem(p, RING)
        for way in range(2):
            s1_copy(kind, p, way).wait_send()
            s2_copy(kind, p, way).wait_send()

        @pl.when(leaves(p))
        def _():
            for way in range(2):
                for half in ((0, 1), (1, 0))[way]:
                    total_of(kind, p, way, half, (g1s.at[way, half, s], g1r.at[way, half, s]), 1)
                    if half == way:
                        for c in g2_copies(kind, p, way):
                            c.start()

    def do_s5(kind, p):
        s, rows = lax.rem(p, RING), pl.ds(0, height(kind))
        far_s = lax.rem(p, 2 * RING)

        @pl.when(leaves(p))
        def _():
            for way in range(2):
                for half in range(2):
                    total_of(kind, p, way, half, (g1s.at[way, half, s], g1r.at[way, half, s]), 0)
                total_of(kind, p, way, way, (g2s.at[way, far_s], g2r.at[way, far_s]), 1)
                total_of(kind, p, way, way, (g2s.at[way, far_s], g2r.at[way, far_s]), 0)

        for half in range(2):
            pltpu.make_async_copy(wnew.at[s, half, rows], wnew.at[s, half, rows], loc_sem.at[half, s]).wait()

    def each(do, p, among=(GU, DOWN, SMALL)):
        for kind, cond in kind_of(p).items():
            if kind in among:
                @pl.when(cond & (p >= 0) & (p < packs))
                def _():
                    do(kind, p)

    deep = 2

    def lagged(do, p, lag):
        each(do, jnp.where(p < deep, p, jnp.where(p < deep + lag, -1, p - lag)))

    def full(p, among=(GU, DOWN, SMALL)):
        each(do_s1, p, among)
        lagged(do_s3, p - 1, 2)

    def half(p):
        lagged(do_s2, p, 1)
        lagged(do_s4, p - 2, 2)
        each(do_s5, p - 6)


    def weight_loads(it):
        b, lay = lax.rem(it, 2), 1 - it // blocks
        cols = pl.ds(block_cols(it), q)
        return (
            pltpu.make_async_copy(wg_hbm.at[lay, :, cols], wgu.at[b, :, pl.ds(0, q)], weight_sem.at[b, 0]),
            pltpu.make_async_copy(wu_hbm.at[lay, :, cols], wgu.at[b, :, pl.ds(q, q)], weight_sem.at[b, 1]),
            pltpu.make_async_copy(wd_hbm.at[lay, cols, :], wdn.at[b], weight_sem.at[b, 2]),
        )

    def tile_loads(a_hbm, d_hbm, t):
        b, rows = lax.rem(t, 2), pl.ds(mult(t * tm, tm), tm)
        return (
            pltpu.make_async_copy(a_hbm.at[rows, :], tiles.at[b, 0], tile_sem.at[b, 0]),
            pltpu.make_async_copy(d_hbm.at[rows, :], tiles.at[b, 1], tile_sem.at[b, 1]),
        )

    def start_tile(layer_1, t):
        @pl.when(layer_1)
        def _():
            for c in tile_loads(a1_hbm, dy_hbm, t):
                c.start()

        @pl.when(jnp.logical_not(layer_1))
        def _():
            for c in tile_loads(a0_hbm, dh_hbm, t):
                c.start()

    def compute(b, wb, t, layer_1):
        a, dh = tiles[b, 0], tiles[b, 1]
        m = tm // 2
        at[...] = a.T
        dht[...] = dh.T
        dact = [dot(dh[r], wdt[...]) for r in (slice(0, m), slice(m, tm))]
        gu = [dot(a[r], wgu[wb]) for r in (slice(0, m), slice(m, tm))]
        for k in range(2):
            rows = slice(k * m, (k + 1) * m)
            gate, up = gu[k][:, :q], gu[k][:, q:]
            dk = dact[k].astype(BF16).astype(F32)
            s = jax.nn.sigmoid(gate)
            silu = gate * s
            act = (silu * up).astype(BF16)
            dup = (dk * silu).astype(BF16)
            dgate = (dk * up * (s + silu * (1 - s))).astype(BF16)
            dgu = jnp.concatenate([dgate, dup], -1)
            if layer_1:
                da[pl.ds(mult(t * tm + k * m, m), m), :] += dot(dgu, wgut[...])
            accgu[...] += dot(at[:, rows], dgu)
            for r in (slice(0, d // 2), slice(d // 2, d)):
                accd[r, :] += dot(dht[r, rows], act)

    part_rows = min(tm, 256)
    quarter = steps // 4

    def between_layers():
        def loads(t):
            return tile_loads(h1_hbm, dy_hbm, t)

        def store(t):
            b = lax.rem(t, 2)
            return pltpu.make_async_copy(tiles.at[b, 1], dh_hbm.at[pl.ds(mult(t * tm, tm), tm), :], hout_sem.at[b])

        for c in loads(0):
            c.start()

        def tile(t, _):
            b = lax.rem(t, 2)
            for c in loads(t):
                c.wait()

            @pl.when(t >= 1)
            def _():
                store(t - 1).wait()

            @pl.when(t + 1 < steps)
            def _():
                for c in loads(t + 1):
                    c.start()

            def part(k, _):
                rows = pl.ds(mult(k * part_rows, part_rows), part_rows)
                g = da[pl.ds(mult(t * tm + k * part_rows, part_rows), part_rows), :].astype(BF16).astype(F32)
                wide = tiles[b, 0, rows, :].astype(F32)
                scale = norm_scale(wide)
                inner = jnp.mean(g * wide, -1, keepdims=True)
                tiles[b, 1, rows, :] = tiles[b, 1, rows, :] + (scale * g - wide * (scale * scale * scale * inner)).astype(BF16)
                return 0

            lax.fori_loop(0, tm // part_rows, part, 0)
            store(t).start()

            @pl.when(t == steps // 2 - 1)
            def _():
                half(pack_of_block(blocks - 1))

            return 0

        lax.fori_loop(0, steps, tile, 0)
        store(steps - 1).wait()

    for c in weight_loads(0):
        c.start()
    start_tile(True, 0)
    da[...] = jnp.zeros_like(da)

    def block(it, _):
        layer_1 = it < blocks
        wb, i = lax.rem(it, 2), lax.rem(it, blocks)
        p = pack_of_block(it)
        with_down = it >= LEAD

        @pl.when(it == blocks)
        def _():
            between_layers()
            start_tile(False, 0)

        for c in weight_loads(it):
            c.wait()

        @pl.when(it + 1 < 2 * blocks)
        def _():
            for c in weight_loads(it + 1):
                c.start()

        wdt[...] = wdn[wb].T

        @pl.when(layer_1)
        def _():
            wgut[...] = wgu[wb].T

        accgu[...] = jnp.zeros_like(accgu)
        accd[...] = jnp.zeros_like(accd)

        def tile(t, _):
            b = lax.rem(t, 2)
            for c in tile_loads(a1_hbm, dy_hbm, t):
                c.wait()

            more = (t + 1 < steps) | ((it + 1 != blocks) & (it + 1 != 2 * blocks))

            @pl.when(more)
            def _():
                start_tile(layer_1, lax.rem(t + 1, steps))

            @pl.when(layer_1)
            def _():
                compute(b, wb, t, True)

            @pl.when(jnp.logical_not(layer_1))
            def _():
                compute(b, wb, t, False)

            @pl.when((t == quarter - 1) & (it >= 1) & (it != blocks))
            def _():
                half(pack_of_block(it - 1))

            @pl.when((t == 2 * quarter - 1) & with_down)
            def _():
                full(p - 1, (DOWN, SMALL))

            @pl.when((t == 3 * quarter - 1) & with_down)
            def _():
                half(p - 1)

            return 0

        lax.fori_loop(0, steps, tile, 0)
        k = jnp.where(i < LEAD, i, lax.rem(jnp.maximum(i - LEAD, 0), 4))
        slot = lax.rem(jnp.where(i < LEAD, 0, (i + 1) // 4) + jnp.where(layer_1, 0, GROUPS), 2)
        for c in range(d // q):
            dbuf[slot, pl.ds(mult(k * q, q), q), c * q : (c + 1) * q] = accd[c * q : (c + 1) * q, :].astype(BF16).T
        full(p, (GU,))
        return 0

    lax.fori_loop(0, 2 * blocks, block, 0)
    end = packs

    def tail(p, _):
        half(p)
        full(p + 1, (DOWN, SMALL))
        return 0

    lax.fori_loop(pairs_end(blocks) - 1, end + 6, tail, 0)
    for p in (end - 2, end - 1):
        moment_stores_wait(DOWN, p)


def backward(a1, dy, h1, a0, wg, wu, wd, moments, n, axis, tm=None):
    tm = tm or TB
    t, d = dy.shape
    ff = wg.shape[-1]
    q = BLOCK
    V = pltpu.VMEM
    DMA = pltpu.SemaphoreType.DMA
    mg, mu, md, vg, vu, vd = moments
    outs = [jax.ShapeDtypeStruct(w.shape, BF16) for w in (wg, wu, wd)]
    outs += [jax.ShapeDtypeStruct(m.shape, F32) for m in moments]
    outs += [jax.ShapeDtypeStruct((t, d), BF16), *[jax.ShapeDtypeStruct((kept_height(), q), BF16)] * 2]
    return pl.pallas_call(
        functools.partial(backward_kernel, n, t // tm, d, ff, axis),
        in_specs=[ANY] * 13,
        out_specs=[ANY] * 12,
        out_shape=outs,
        scratch_shapes=[
            V((2, 2, tm, d), BF16),
            V((d, tm), BF16),
            V((d, tm), BF16),
            V((2, d, 2 * q), BF16),
            V((2, q, d), BF16),
            V((d, q), BF16),
            V((2 * q, d), BF16),
            V((d, 2 * q), F32),
            V((d, q), F32),
            V((t, d), F32),
            V((2, 4 * q, d), BF16),
            V((RING, 2, 2 * q, q), BF16),
            V((KEEP_RING, 2, q, q), BF16),
            V((OWN_RING, 2, q, q), BF16),
            V((RING, 2, 2 * q, q), BF16),
            V((RING, 2, q, q), BF16),
            V((RING, 2, q, q), BF16),
            V((RING, 2, q, q), BF16),
            V((2, 4, q, q), F32),
            V((2, 2, q, q), BF16),
            V((2, 4, q, q), F32),
            DMA((2, 2)),
            DMA((2, 3)),
            DMA((2,)),
            DMA((2, RING)),
            DMA((2, RING)),
            DMA((2, RING)),
            DMA((2, RING)),
            DMA((2, 2, RING)),
            DMA((2, 2, RING)),
            DMA((2, 2 * RING)),
            DMA((2, 2 * RING)),
            DMA((2, RING)),
            DMA((2, 6)),
            DMA((2, 4)),
        ],
        compiler_params=pltpu.CompilerParams(vmem_limit_bytes=67_043_328, collective_id=0, has_side_effects=True),
        cost_estimate=pl.CostEstimate(flops=28 * t * d * ff, bytes_accessed=44 * t * d, transcendentals=2 * t * ff),
        name="backward",
    )(a1, dy, h1, a0, wg, wu, wd, *moments)


def kept_height():
    return 4 * BLOCK + 8 * (BLOCK // 2)


def results_kernel(count, rows, *refs):
    sources, rest = refs[:count], refs[count + 1 :]
    outs, rest = rest[:count], rest[count:]
    kinds = []
    for r in sources:
        if (key := (r.shape[1:], r.dtype)) not in kinds:
            kinds.append(key)
    buffers, (isem, osem) = rest[: len(kinds)], rest[len(kinds) :]
    steps, used = [], [0] * len(kinds)
    for k, r in enumerate(sources):
        kind = kinds.index((r.shape[1:], r.dtype))
        size = buffers[kind].shape[1]
        for lay in range(r.shape[0]):
            for at_ in range(0, r.shape[1], size):
                steps.append((k, kind, used[kind] % SLOTS, lay, at_, size))
                used[kind] += 1

    def copy_in(step):
        k, kind, slot, lay, at_, size = steps[step]
        return pltpu.make_async_copy(sources[k].at[lay, pl.ds(at_, size)], buffers[kind].at[slot], isem.at[kind, slot])

    def copy_out(step):
        k, kind, slot, lay, at_, size = steps[step]
        return pltpu.make_async_copy(buffers[kind].at[slot], outs[k].at[lay, pl.ds(at_, size)], osem.at[kind, slot])

    flying = {}

    def start_in(step):
        key = steps[step][1:3]
        if key in flying:
            copy_out(flying.pop(key)).wait()
        copy_in(step).start()

    for step in range(min(AHEAD, len(steps))):
        start_in(step)
    for step in range(len(steps)):
        copy_in(step).wait()
        copy_out(step).start()
        flying[steps[step][1:3]] = step
        if step + AHEAD < len(steps):
            start_in(step + AHEAD)
    for step in flying.values():
        copy_out(step).wait()


def results(sources, token):
    piece = 128 * 2816 * 2
    kinds = []
    for r in sources:
        if (key := (r.shape[1:], r.dtype)) not in kinds:
            kinds.append(key)
    buffers = []
    for (_, width), dtype in kinds:
        buffers.append(pltpu.VMEM((SLOTS, piece // (width * dtype.itemsize), width), dtype))
    size = sum(r.size * r.dtype.itemsize for r in sources)
    return pl.pallas_call(
        functools.partial(results_kernel, len(sources), None),
        in_specs=[ANY] * (len(sources) + 1),
        out_specs=[ANY] * len(sources),
        out_shape=[jax.ShapeDtypeStruct(r.shape, r.dtype) for r in sources],
        scratch_shapes=buffers + [pltpu.SemaphoreType.DMA((len(kinds), SLOTS))] * 2,
        compiler_params=pltpu.CompilerParams(vmem_limit_bytes=62 * MIB),
        cost_estimate=pl.CostEstimate(flops=20 * 10**9, bytes_accessed=2 * size, transcendentals=0),
        name="results",
    )(*sources, token)


def kept_kernel(n, axis, blocks, away, *refs):
    halves, (ng_out, nu_out, nd_out, sem) = refs[: 2 * len(away)], refs[2 * len(away) + 3 :]
    q, u = BLOCK, UNIT
    small = q // 2
    pair = q + small
    me = lax.axis_index(axis)
    ff = nd_out.shape[1]
    mult = pl.multiple_of
    copies = []

    def put(src, dst):
        copies.append(pltpu.make_async_copy(src, dst, sem.at[len(copies)]))

    for k, src in enumerate(halves):
        dev, half = lax.rem(me + away[k // 2], n), k % 2
        base = dev * (ff // n)
        out = (ng_out, nu_out)[half]
        rows = pl.ds(mult(dev * q, q), q)
        for b in range(4):
            put(src.at[pl.ds(b * pair, q)], out.at[0, rows, pl.ds(block_of(blocks - 4 + b) * q, q)])
        for b in range(8):
            at_ = b * pair + q if b < 4 else 4 * pair + (b - 4) * small
            row = pl.ds(mult(base + b // 4 * 4 * u + dev * u + half * small, u), small)
            put(src.at[pl.ds(at_, small)], nd_out.at[0, row, pl.ds(b % 4 * q, q)])
    for c in copies:
        c.start()
    for c in copies:
        c.wait()


def place_kept(parts, away, weights, n, axis):
    blocks = weights[0].shape[-1] // BLOCK
    vmem = pl.BlockSpec(memory_space=pltpu.VMEM)
    count = len(parts)
    return pl.pallas_call(
        functools.partial(kept_kernel, n, axis, blocks, away),
        in_specs=[vmem] * count + [ANY] * 3,
        out_specs=[ANY] * 3,
        out_shape=[jax.ShapeDtypeStruct(w.shape, w.dtype) for w in weights],
        input_output_aliases={count + k: k for k in range(3)},
        scratch_shapes=[pltpu.SemaphoreType.DMA((count * 12,))],
        compiler_params=pltpu.CompilerParams(vmem_limit_bytes=62 * MIB),
        cost_estimate=pl.CostEstimate(flops=10**9, bytes_accessed=count * 4 * MIB, transcendentals=0),
        name="place_kept",
    )(*parts, *weights)


def solution(mesh):
    n = mesh.shape["dp"]
    to_right = [(k, (k + 1) % n) for k in range(n)]
    to_left = [(k, (k - 1) % n) for k in range(n)]

    def step(x, dy, wg, wu, wd, m_g, m_u, m_d, v_g, v_u, v_d):
        x, dy = x[0], dy[0]
        a0, h1, a1 = forward(x, wg, wu, wd)
        ng, nu, nd, mg, mu, md, vg, vu, vd, _, a, b = backward(a1, dy, h1, a0, wg, wu, wd, (m_g, m_u, m_d, v_g, v_u, v_d), n, "dp")
        la, rb = lax.ppermute(a, "dp", to_right), lax.ppermute(b, "dp", to_left)
        mg, mu, vg, vu = results((mg, mu, vg, vu), a)
        a, b, mg = lax.optimization_barrier((a, b, mg))
        lb, ra = lax.ppermute(b, "dp", to_right), lax.ppermute(a, "dp", to_left)
        md, vd, nd = results((md, vd, nd), mg)
        la, rb, md = lax.optimization_barrier((la, rb, md))
        fa, fb = lax.ppermute(la, "dp", to_right), lax.ppermute(rb, "dp", to_left)
        ng, nu = results((ng, nu), md)
        new = place_kept((a, b, ra, rb, la, lb), (0, 1, n - 1), (ng, nu, nd), n, "dp")
        new = place_kept((fa, fb), (2,), new, n, "dp")
        return (*new, mg, mu, md, vg, vu, vd)

    seq = P(("rep", "dp"), None, None)
    rows = P(None, "dp", None)
    whole = P("rep", None, None)
    part = P("rep", "dp", None)
    return jax.shard_map(
        step,
        mesh=mesh,
        in_specs=(seq, seq, P(), P(), P()) + (rows,) * 6,
        out_specs=(whole,) * 3 + (part,) * 6,
        check_vma=False,
    )
```

```python
import functools

import jax
import jax.numpy as jnp
from jax import lax
from jax.experimental import pallas as pl
from jax.experimental.pallas import tpu as pltpu
from jax.sharding import PartitionSpec as P

F32, BF16 = jnp.float32, jnp.bfloat16
BLOCK = 256
UNIT = 64
MIB = 2**20
TM = 512
TB = 1024
ANY = pl.BlockSpec(memory_space=pl.ANY)


def dot(a, b):
    return jnp.dot(a, b, preferred_element_type=F32)


def norm_scale(wide):
    return lax.rsqrt(jnp.mean(wide * wide, -1, keepdims=True) + 1e-6)


def params(limit=60):
    return pltpu.CompilerParams(vmem_limit_bytes=limit * MIB, dimension_semantics=("arbitrary",))


def forward_kernel(blocks, x_ref, wg_hbm, wu_hbm, wd_hbm, a0_ref, h_ref, a1_ref, wg, wu, wd, act, sems):
    step = pl.program_id(0)

    def copies(b):
        cols = pl.ds(b * BLOCK, BLOCK)
        return (
            pltpu.make_async_copy(wg_hbm.at[0, :, cols], wg.at[:, cols], sems.at[0, b]),
            pltpu.make_async_copy(wu_hbm.at[0, :, cols], wu.at[:, cols], sems.at[1, b]),
            pltpu.make_async_copy(wd_hbm.at[0, cols, :], wd.at[cols, :], sems.at[2, b]),
        )

    @pl.when(step == 0)
    def _():
        for b in range(blocks):
            for c in copies(b):
                c.start()

    tm = x_ref.shape[0]
    halves = (slice(0, tm // 2), slice(tm // 2, tm))

    def hidden(rows, cols):
        gate = dot(a0_ref[rows, :], wg[:, cols])
        up = dot(a0_ref[rows, :], wu[:, cols])
        act[rows, cols] = (gate * jax.nn.sigmoid(gate) * up).astype(BF16)

    def norm(rows):
        wide = x_ref[rows, :].astype(F32)
        a0_ref[rows, :] = (wide * norm_scale(wide)).astype(BF16)

    def first():
        norm(slice(0, tm))

        def block(b, _):
            for c in copies(b)[:2]:
                c.wait()
            hidden(slice(0, tm), pl.ds(pl.multiple_of(b * BLOCK, BLOCK), BLOCK))
            return 0

        lax.fori_loop(0, blocks, block, 0)
        for b in range(blocks):
            copies(b)[2].wait()

    def finish(rows):
        h = x_ref[rows, :] + dot(act[rows, :], wd[...]).astype(BF16)
        h_ref[rows, :] = h
        wide = h.astype(F32)
        a1_ref[rows, :] = (wide * norm_scale(wide)).astype(BF16)

    @pl.when(step == 0)
    def _():
        first()
        for rows in halves:
            finish(rows)

    @pl.when(step > 0)
    def _():
        for rows in halves:
            norm(rows)
            for b in range(blocks):
                hidden(rows, slice(b * BLOCK, (b + 1) * BLOCK))
        for rows in halves:
            finish(rows)


def forward(x, wg, wu, wd, tm=None):
    tm = tm or TM
    t, d = x.shape
    ff = wg.shape[-1]
    blocks = ff // BLOCK
    tile = pl.BlockSpec((tm, d), lambda i: (i, 0))
    return pl.pallas_call(
        functools.partial(forward_kernel, blocks),
        grid=(t // tm,),
        in_specs=[tile, ANY, ANY, ANY],
        out_specs=[tile] * 3,
        out_shape=[jax.ShapeDtypeStruct((t, d), BF16)] * 3,
        scratch_shapes=[
            pltpu.VMEM((d, ff), BF16),
            pltpu.VMEM((d, ff), BF16),
            pltpu.VMEM((ff, d), BF16),
            pltpu.VMEM((tm, ff), BF16),
            pltpu.SemaphoreType.DMA((3, blocks)),
        ],
        compiler_params=params(),
        cost_estimate=pl.CostEstimate(flops=6 * t * d * ff, bytes_accessed=8 * t * d + 6 * d * ff, transcendentals=t * ff),
        name="forward",
    )(x, wg, wu, wd)


def adamw(w, m, v, g):
    m = 0.9 * m + 0.1 * g
    v = 0.95 * v + 0.05 * g * g
    step = m * lax.rsqrt(v + 1e-8) + 0.1 * w
    return (w - 0.02 * step).astype(BF16), m, v


GU, DOWN, SMALL = 0, 1, 2
RING = 6
KEEP_RING = 3
OWN_RING = 4
LEAD = 3
QUARTERS = 4
GROUPS = 3
KEPT = 12
SLOTS = 12
AHEAD = 6


def pack_of_block(it):
    return jnp.where(it < LEAD, it, 2 * it - LEAD + 1)


def pairs_end(blocks):
    return 4 * blocks - LEAD


def pack_kind(p, blocks):
    down = ((p >= LEAD) & (p < pairs_end(blocks)) & (lax.rem(p + LEAD, 2) == 0)) | (p >= pairs_end(blocks))
    small = down & (lax.rem(pack_down(p, blocks) // QUARTERS, GROUPS) == 0)
    return {GU: jnp.logical_not(down), DOWN: down & jnp.logical_not(small), SMALL: small}


def pack_block(p):
    return jnp.where(p < LEAD, p, (p + LEAD - 1) // 2)


def pack_down(p, blocks):
    return jnp.where(p < pairs_end(blocks), jnp.maximum(p - LEAD, 0) // 2, p - 2 * blocks)


def block_of(i):
    j = i - LEAD
    if isinstance(i, int):
        return 3 * i + 2 if i < LEAD else 3 * (j % 4) + j // 4
    j = jnp.maximum(j, 0)
    return jnp.where(i < LEAD, 3 * i + 2, 3 * lax.rem(j, 4) + j // 4)


def backward_kernel(
    n, steps, d, ff, axis,
    a1_hbm, dy_hbm, h1_hbm, a0_hbm, wg_hbm, wu_hbm, wd_hbm, mg_hbm, mu_hbm, md_hbm, vg_hbm, vu_hbm, vd_hbm,
    ng_hbm, nu_hbm, nd_hbm, mg_out, mu_out, md_out, vg_out, vu_out, vd_out, dh_hbm, kept_a, kept_b,
    tiles, at, dht, wgu, wdn, wdt, wgut, accgu, accd, da, dbuf,
    send, keep, own, r1, r2, s2, wnew, mvin, win, mvout,
    tile_sem, weight_sem, hout_sem, s1s, s1r, s2s, s2r, g1s, g1r, g2s, g2r, loc_sem, mvin_sem, mvout_sem,
):
    tm = tiles.shape[2]
    blocks = ff // BLOCK
    packs = 2 * blocks + 2 * GROUPS * QUARTERS
    q = BLOCK
    me = lax.axis_index(axis)
    right, left, far = (lax.rem(me + k, n) for k in (1, n - 1, 2))
    to = ({axis: right}, {axis: left})
    mult = pl.multiple_of

    barrier = pltpu.get_barrier_semaphore()
    for dev in to:
        pl.semaphore_signal(barrier, inc=1, device_id=dev, device_id_type=pl.DeviceIdType.MESH)
    pl.semaphore_wait(barrier, 2)


    kind_of = functools.partial(pack_kind, blocks=blocks)

    def block_cols(it):
        return mult(block_of(lax.rem(it, blocks)) * q, q)

    def down_group(p):
        return pack_down(p, blocks) // QUARTERS

    def down_cols(p):
        return mult(lax.rem(pack_down(p, blocks), QUARTERS) * q, q)

    def height(kind):
        return {GU: q, DOWN: q // 2, SMALL: 3 * UNIT // 2}[kind]

    def last_row(dev, k):
        u = k // 2
        return mult(jnp.where(u < dev, u * UNIT, 8 * UNIT + u * UNIT) + (k % 2) * (UNIT // 2), UNIT // 2)

    def rows_in(kind, p, dev, half, ref_gu, ref_d, per_device):
        if kind == GU:
            it = pack_block(p)
            base = 0 if per_device else mult(dev * q, q)
            return [(ref_gu[half].at[1 - it // blocks, pl.ds(base, q), pl.ds(block_cols(it), q)], 0, q)]
        group = down_group(p)
        lay, cols = 1 - group // GROUPS, pl.ds(down_cols(p), q)
        base = 0 if per_device else dev * (ff // n)
        if kind == DOWN:
            row = base + (lax.rem(group, GROUPS) - 1) * 4 * UNIT + dev * UNIT + half * (q // 2)
            return [(ref_d.at[lay, pl.ds(mult(row, UNIT), q // 2), cols], 0, q // 2)]
        small = UNIT // 2
        return [
            (ref_d.at[lay, pl.ds(mult(base + last_row(dev, 3 * half + k), small), small), cols], k * small, small) for k in range(3)
        ]

    def kept_rows(kind, p):
        k = p - (packs - KEPT)
        small = q // 2
        pair = q + small
        if kind == GU:
            row = k // 2 * pair
        else:
            row = jnp.where(k < 8, k // 2 * pair + q, 4 * pair + (k - 8) * small)
        return pl.ds(mult(row, UNIT // 2), height(kind))

    def new_pieces(kind, p, dev, half):
        return rows_in(kind, p, dev, half, (ng_hbm, nu_hbm), nd_hbm, False)


    def s1_copy(kind, p, way):
        s, h = lax.rem(p, RING), height(kind)
        rows = pl.ds(0, 2 * h)
        return pltpu.make_async_remote_copy(
            send.at[s, way, rows], r1.at[s, way, rows], s1s.at[way, s], s1r.at[way, s], to[way], pl.DeviceIdType.MESH
        )

    def s2_copy(kind, p, way):
        s, h = lax.rem(p, RING), height(kind)
        rows = pl.ds(0, h)
        return pltpu.make_async_remote_copy(
            s2.at[s, way, rows], r2.at[s, way, rows], s2s.at[way, s], s2r.at[way, s], to[way], pl.DeviceIdType.MESH
        )

    def g1_copies(kind, p, way, half):
        s = lax.rem(p, RING)
        return [
            pltpu.make_async_remote_copy(
                wnew.at[s, half, pl.ds(at_, size)], view, g1s.at[way, half, s], g1r.at[way, half, s], to[way], pl.DeviceIdType.MESH
            )
            for view, at_, size in new_pieces(kind, p, me, half)
        ]

    def g2_copies(kind, p, way):
        s, dev = lax.rem(p, 2 * RING), (left, right)[way]
        return [
            pltpu.make_async_remote_copy(view, view, g2s.at[way, s], g2r.at[way, s], to[way], pl.DeviceIdType.MESH)
            for view, _, _ in new_pieces(kind, p, dev, way)
        ]

    def total_of(kind, p, way, half, sems, side):
        s, h = lax.rem(p, RING), height(kind)
        ref = wnew.at[s, half, pl.ds(0, h)]
        copy = pltpu.make_async_remote_copy(ref, ref, sems[0], sems[1], to[way], pl.DeviceIdType.MESH)
        copy.wait_send() if side == 0 else copy.wait_recv()

    def moment_loads(kind, p):
        b, s = lax.rem(p, 2), []
        for half in range(2):
            for k, (gu, dn) in enumerate((((mg_hbm, mu_hbm), md_hbm), ((vg_hbm, vu_hbm), vd_hbm))):
                for view, at_, size in rows_in(kind, p, me, half, gu, dn, True):
                    s.append(pltpu.make_async_copy(view, mvin.at[b, 2 * half + k, pl.ds(at_, size)], mvin_sem.at[b, 2 * half + k]))
            for view, at_, size in rows_in(kind, p, me, half, (wg_hbm, wu_hbm), wd_hbm, False):
                s.append(pltpu.make_async_copy(view, win.at[b, half, pl.ds(at_, size)], mvin_sem.at[b, 4 + half]))
        return s

    def moment_loads_wait(kind, p):
        b, rows = lax.rem(p, 2), pl.ds(0, height(kind))
        for k in range(4):
            pltpu.make_async_copy(mvin.at[b, k, rows], mvin.at[b, k, rows], mvin_sem.at[b, k]).wait()
        for half in range(2):
            pltpu.make_async_copy(win.at[b, half, rows], win.at[b, half, rows], mvin_sem.at[b, 4 + half]).wait()

    def moment_stores(kind, p):
        b, s = lax.rem(p, 2), []
        for half in range(2):
            for k, (gu, dn) in enumerate((((mg_out, mu_out), md_out), ((vg_out, vu_out), vd_out))):
                for view, at_, size in rows_in(kind, p, me, half, gu, dn, True):
                    s.append(pltpu.make_async_copy(mvout.at[b, 2 * half + k, pl.ds(at_, size)], view, mvout_sem.at[b, 2 * half + k]))
        return s

    def moment_stores_wait(kind, p):
        b, rows = lax.rem(p, 2), pl.ds(0, height(kind))
        for k in range(4):
            pltpu.make_async_copy(mvout.at[b, k, rows], mvout.at[b, k, rows], mvout_sem.at[b, k]).wait()

    def own_copies(kind, p):
        s = lax.rem(p, RING)
        return [
            pltpu.make_async_copy(wnew.at[s, half, pl.ds(at_, size)], view, loc_sem.at[half, s])
            for half in range(2)
            for view, at_, size in new_pieces(kind, p, me, half)
        ]

    def kept_copies(kind, p):
        s, h = lax.rem(p, RING), height(kind)
        return [
            pltpu.make_async_copy(wnew.at[s, half, pl.ds(0, h)], (kept_a, kept_b)[half].at[kept_rows(kind, p)], loc_sem.at[half, s]) for half in range(2)
        ]

    def leaves(p):
        return p < packs - KEPT

    def stage(kind, p):
        s, h = lax.rem(p, RING), height(kind)
        if kind == GU:
            def part(dev, half):
                return accgu[pl.ds(mult(dev * q, q), q), half * q : (half + 1) * q].astype(BF16)
        else:
            slot = lax.rem(down_group(p), 2)

            def part(dev, half):
                return dbuf[slot, pl.ds(mult(dev * (2 * h) + half * h, UNIT // 2), h), pl.ds(down_cols(p), q)]
        send[s, 0, :h, :] = part(far, 0)
        send[s, 0, h : 2 * h, :] = part(right, 1)
        send[s, 1, :h, :] = part(far, 1)
        send[s, 1, h : 2 * h, :] = part(left, 0)
        sk, so = lax.rem(p, KEEP_RING), lax.rem(p, OWN_RING)
        keep[sk, 0, :h, :] = part(right, 0)
        keep[sk, 1, :h, :] = part(left, 1)
        own[so, 0, :h, :] = part(me, 0)
        own[so, 1, :h, :] = part(me, 1)

    def do_s1(kind, p):
        stage(kind, p)
        for way in range(2):
            s1_copy(kind, p, way).start()

    def do_s2(kind, p):
        s, h = lax.rem(p, RING), height(kind)
        for c in moment_loads(kind, p):
            c.start()
        for way in range(2):
            s1_copy(kind, p, way).wait_recv()
            s2[s, way, :h, :] = (keep[lax.rem(p, KEEP_RING), way, :h, :].astype(F32) + r1[s, way, :h, :].astype(F32)).astype(BF16)
            s2_copy(kind, p, way).start()

    def do_s3(kind, p):
        s, b, h = lax.rem(p, RING), lax.rem(p, 2), height(kind)
        grain = h if kind == SMALL else UNIT * 2
        moment_loads_wait(kind, p)
        for k, cond in kind_of(p - 2).items():
            @pl.when(cond & (p >= 2))
            def _():
                moment_stores_wait(k, p - 2)
        for way in range(2):
            s2_copy(kind, p, way).wait_recv()

        def rows_of(u, _):
            rows = pl.ds(mult(u * grain, grain), grain)
            rest = pl.ds(mult(h + u * grain, UNIT // 2), grain)
            for half in range(2):
                g = own[lax.rem(p, OWN_RING), half, rows, :].astype(F32) + r1[s, 1 - half, rest, :].astype(F32) + r2[s, half, rows, :].astype(F32)
                g = g.astype(BF16).astype(F32)
                w, m, v = adamw(win[b, half, rows, :].astype(F32), mvin[b, 2 * half, rows, :], mvin[b, 2 * half + 1, rows, :], g)
                wnew[s, half, rows, :] = w
                mvout[b, 2 * half, rows, :] = m
                mvout[b, 2 * half + 1, rows, :] = v
            return 0

        lax.fori_loop(0, h // grain, rows_of, 0)
        for c in moment_stores(kind, p):
            c.start()

        @pl.when(leaves(p))
        def _():
            for way in range(2):
                for half in ((0, 1), (1, 0))[way]:
                    for c in g1_copies(kind, p, way, half):
                        c.start()
            for c in own_copies(kind, p):
                c.start()

        if kind != SMALL:
            @pl.when(jnp.logical_not(leaves(p)))
            def _():
                for c in kept_copies(kind, p):
                    c.start()

    def do_s4(kind, p):
        s = lax.rem(p, RING)
        for way in range(2):
            s1_copy(kind, p, way).wait_send()
            s2_copy(kind, p, way).wait_send()

        @pl.when(leaves(p))
        def _():
            for way in range(2):
                for half in ((0, 1), (1, 0))[way]:
                    total_of(kind, p, way, half, (g1s.at[way, half, s], g1r.at[way, half, s]), 1)
                    if half == way:
                        for c in g2_copies(kind, p, way):
                            c.start()

    def do_s5(kind, p):
        s, rows = lax.rem(p, RING), pl.ds(0, height(kind))
        far_s = lax.rem(p, 2 * RING)

        @pl.when(leaves(p))
        def _():
            for way in range(2):
                for half in range(2):
                    total_of(kind, p, way, half, (g1s.at[way, half, s], g1r.at[way, half, s]), 0)
                total_of(kind, p, way, way, (g2s.at[way, far_s], g2r.at[way, far_s]), 1)
                total_of(kind, p, way, way, (g2s.at[way, far_s], g2r.at[way, far_s]), 0)

        for half in range(2):
            pltpu.make_async_copy(wnew.at[s, half, rows], wnew.at[s, half, rows], loc_sem.at[half, s]).wait()

    def each(do, p, among=(GU, DOWN, SMALL)):
        for kind, cond in kind_of(p).items():
            if kind in among:
                @pl.when(cond & (p >= 0) & (p < packs))
                def _():
                    do(kind, p)

    deep = 2

    def lagged(do, p, lag):
        each(do, jnp.where(p < deep, p, jnp.where(p < deep + lag, -1, p - lag)))

    def full(p, among=(GU, DOWN, SMALL)):
        each(do_s1, p, among)
        lagged(do_s3, p - 1, 2)

    def half(p):
        lagged(do_s2, p, 1)
        lagged(do_s4, p - 2, 2)
        each(do_s5, p - 6)


    def weight_loads(it):
        b, lay = lax.rem(it, 2), 1 - it // blocks
        cols = pl.ds(block_cols(it), q)
        return (
            pltpu.make_async_copy(wg_hbm.at[lay, :, cols], wgu.at[b, :, pl.ds(0, q)], weight_sem.at[b, 0]),
            pltpu.make_async_copy(wu_hbm.at[lay, :, cols], wgu.at[b, :, pl.ds(q, q)], weight_sem.at[b, 1]),
            pltpu.make_async_copy(wd_hbm.at[lay, cols, :], wdn.at[b], weight_sem.at[b, 2]),
        )

    def tile_loads(a_hbm, d_hbm, t):
        b, rows = lax.rem(t, 2), pl.ds(mult(t * tm, tm), tm)
        return (
            pltpu.make_async_copy(a_hbm.at[rows, :], tiles.at[b, 0], tile_sem.at[b, 0]),
            pltpu.make_async_copy(d_hbm.at[rows, :], tiles.at[b, 1], tile_sem.at[b, 1]),
        )

    def start_tile(layer_1, t):
        @pl.when(layer_1)
        def _():
            for c in tile_loads(a1_hbm, dy_hbm, t):
                c.start()

        @pl.when(jnp.logical_not(layer_1))
        def _():
            for c in tile_loads(a0_hbm, dh_hbm, t):
                c.start()

    def compute(b, wb, t, layer_1):
        a, dh = tiles[b, 0], tiles[b, 1]
        m = tm // 2
        at[...] = a.T
        dht[...] = dh.T
        dact = [dot(dh[r], wdt[...]) for r in (slice(0, m), slice(m, tm))]
        gu = [dot(a[r], wgu[wb]) for r in (slice(0, m), slice(m, tm))]
        for k in range(2):
            rows = slice(k * m, (k + 1) * m)
            gate, up = gu[k][:, :q], gu[k][:, q:]
            dk = dact[k].astype(BF16).astype(F32)
            s = jax.nn.sigmoid(gate)
            silu = gate * s
            act = (silu * up).astype(BF16)
            dup = (dk * silu).astype(BF16)
            dgate = (dk * up * (s + silu * (1 - s))).astype(BF16)
            dgu = jnp.concatenate([dgate, dup], -1)
            if layer_1:
                da[pl.ds(mult(t * tm + k * m, m), m), :] += dot(dgu, wgut[...])
            accgu[...] += dot(at[:, rows], dgu)
            for r in (slice(0, d // 2), slice(d // 2, d)):
                accd[r, :] += dot(dht[r, rows], act)

    part_rows = min(tm, 256)
    quarter = steps // 4

    def between_layers():
        def loads(t):
            return tile_loads(h1_hbm, dy_hbm, t)

        def store(t):
            b = lax.rem(t, 2)
            return pltpu.make_async_copy(tiles.at[b, 1], dh_hbm.at[pl.ds(mult(t * tm, tm), tm), :], hout_sem.at[b])

        for c in loads(0):
            c.start()

        def tile(t, _):
            b = lax.rem(t, 2)
            for c in loads(t):
                c.wait()

            @pl.when(t >= 1)
            def _():
                store(t - 1).wait()

            @pl.when(t + 1 < steps)
            def _():
                for c in loads(t + 1):
                    c.start()

            def part(k, _):
                rows = pl.ds(mult(k * part_rows, part_rows), part_rows)
                g = da[pl.ds(mult(t * tm + k * part_rows, part_rows), part_rows), :].astype(BF16).astype(F32)
                wide = tiles[b, 0, rows, :].astype(F32)
                scale = norm_scale(wide)
                inner = jnp.mean(g * wide, -1, keepdims=True)
                tiles[b, 1, rows, :] = tiles[b, 1, rows, :] + (scale * g - wide * (scale * scale * scale * inner)).astype(BF16)
                return 0

            lax.fori_loop(0, tm // part_rows, part, 0)
            store(t).start()

            @pl.when(t == steps // 2 - 1)
            def _():
                half(pack_of_block(blocks - 1))

            return 0

        lax.fori_loop(0, steps, tile, 0)
        store(steps - 1).wait()

    for c in weight_loads(0):
        c.start()
    start_tile(True, 0)
    da[...] = jnp.zeros_like(da)

    def block(it, _):
        layer_1 = it < blocks
        wb, i = lax.rem(it, 2), lax.rem(it, blocks)
        p = pack_of_block(it)
        with_down = it >= LEAD

        @pl.when(it == blocks)
        def _():
            between_layers()
            start_tile(False, 0)

        for c in weight_loads(it):
            c.wait()

        @pl.when(it + 1 < 2 * blocks)
        def _():
            for c in weight_loads(it + 1):
                c.start()

        wdt[...] = wdn[wb].T

        @pl.when(layer_1)
        def _():
            wgut[...] = wgu[wb].T

        accgu[...] = jnp.zeros_like(accgu)
        accd[...] = jnp.zeros_like(accd)

        def tile(t, _):
            b = lax.rem(t, 2)
            for c in tile_loads(a1_hbm, dy_hbm, t):
                c.wait()

            more = (t + 1 < steps) | ((it + 1 != blocks) & (it + 1 != 2 * blocks))

            @pl.when(more)
            def _():
                start_tile(layer_1, lax.rem(t + 1, steps))

            @pl.when(layer_1)
            def _():
                compute(b, wb, t, True)

            @pl.when(jnp.logical_not(layer_1))
            def _():
                compute(b, wb, t, False)

            @pl.when((t == quarter - 1) & (it >= 1) & (it != blocks))
            def _():
                half(pack_of_block(it - 1))

            @pl.when((t == 2 * quarter - 1) & with_down)
            def _():
                full(p - 1, (DOWN, SMALL))

            @pl.when((t == 3 * quarter - 1) & with_down)
            def _():
                half(p - 1)

            return 0

        lax.fori_loop(0, steps, tile, 0)
        k = jnp.where(i < LEAD, i, lax.rem(jnp.maximum(i - LEAD, 0), 4))
        slot = lax.rem(jnp.where(i < LEAD, 0, (i + 1) // 4) + jnp.where(layer_1, 0, GROUPS), 2)
        for c in range(d // q):
            dbuf[slot, pl.ds(mult(k * q, q), q), c * q : (c + 1) * q] = accd[c * q : (c + 1) * q, :].astype(BF16).T
        full(p, (GU,))
        return 0

    lax.fori_loop(0, 2 * blocks, block, 0)
    end = packs

    def tail(p, _):
        half(p)
        full(p + 1, (DOWN, SMALL))
        return 0

    lax.fori_loop(pairs_end(blocks) - 1, end + 6, tail, 0)
    for p in (end - 2, end - 1):
        moment_stores_wait(DOWN, p)


def backward(a1, dy, h1, a0, wg, wu, wd, moments, n, axis, tm=None):
    tm = tm or TB
    t, d = dy.shape
    ff = wg.shape[-1]
    q = BLOCK
    V = pltpu.VMEM
    DMA = pltpu.SemaphoreType.DMA
    mg, mu, md, vg, vu, vd = moments
    outs = [jax.ShapeDtypeStruct(w.shape, BF16) for w in (wg, wu, wd)]
    outs += [jax.ShapeDtypeStruct(m.shape, F32) for m in moments]
    outs += [jax.ShapeDtypeStruct((t, d), BF16), *[jax.ShapeDtypeStruct((kept_height(), q), BF16)] * 2]
    return pl.pallas_call(
        functools.partial(backward_kernel, n, t // tm, d, ff, axis),
        in_specs=[ANY] * 13,
        out_specs=[ANY] * 12,
        out_shape=outs,
        scratch_shapes=[
            V((2, 2, tm, d), BF16),
            V((d, tm), BF16),
            V((d, tm), BF16),
            V((2, d, 2 * q), BF16),
            V((2, q, d), BF16),
            V((d, q), BF16),
            V((2 * q, d), BF16),
            V((d, 2 * q), F32),
            V((d, q), F32),
            V((t, d), F32),
            V((2, 4 * q, d), BF16),
            V((RING, 2, 2 * q, q), BF16),
            V((KEEP_RING, 2, q, q), BF16),
            V((OWN_RING, 2, q, q), BF16),
            V((RING, 2, 2 * q, q), BF16),
            V((RING, 2, q, q), BF16),
            V((RING, 2, q, q), BF16),
            V((RING, 2, q, q), BF16),
            V((2, 4, q, q), F32),
            V((2, 2, q, q), BF16),
            V((2, 4, q, q), F32),
            DMA((2, 2)),
            DMA((2, 3)),
            DMA((2,)),
            DMA((2, RING)),
            DMA((2, RING)),
            DMA((2, RING)),
            DMA((2, RING)),
            DMA((2, 2, RING)),
            DMA((2, 2, RING)),
            DMA((2, 2 * RING)),
            DMA((2, 2 * RING)),
            DMA((2, RING)),
            DMA((2, 6)),
            DMA((2, 4)),
        ],
        compiler_params=pltpu.CompilerParams(vmem_limit_bytes=67_043_328, collective_id=0, has_side_effects=True),
        cost_estimate=pl.CostEstimate(flops=28 * t * d * ff, bytes_accessed=44 * t * d, transcendentals=2 * t * ff),
        name="backward",
    )(a1, dy, h1, a0, wg, wu, wd, *moments)


def kept_height():
    return 4 * BLOCK + 8 * (BLOCK // 2)


def results_kernel(count, rows, *refs):
    sources, rest = refs[:count], refs[count + 1 :]
    outs, rest = rest[:count], rest[count:]
    kinds = []
    for r in sources:
        if (key := (r.shape[1:], r.dtype)) not in kinds:
            kinds.append(key)
    buffers, (isem, osem) = rest[: len(kinds)], rest[len(kinds) :]
    steps, used = [], [0] * len(kinds)
    for k, r in enumerate(sources):
        kind = kinds.index((r.shape[1:], r.dtype))
        size = buffers[kind].shape[1]
        for lay in range(r.shape[0]):
            for at_ in range(0, r.shape[1], size):
                steps.append((k, kind, used[kind] % SLOTS, lay, at_, size))
                used[kind] += 1

    def copy_in(step):
        k, kind, slot, lay, at_, size = steps[step]
        return pltpu.make_async_copy(sources[k].at[lay, pl.ds(at_, size)], buffers[kind].at[slot], isem.at[kind, slot])

    def copy_out(step):
        k, kind, slot, lay, at_, size = steps[step]
        return pltpu.make_async_copy(buffers[kind].at[slot], outs[k].at[lay, pl.ds(at_, size)], osem.at[kind, slot])

    flying = {}

    def start_in(step):
        key = steps[step][1:3]
        if key in flying:
            copy_out(flying.pop(key)).wait()
        copy_in(step).start()

    for step in range(min(AHEAD, len(steps))):
        start_in(step)
    for step in range(len(steps)):
        copy_in(step).wait()
        copy_out(step).start()
        flying[steps[step][1:3]] = step
        if step + AHEAD < len(steps):
            start_in(step + AHEAD)
    for step in flying.values():
        copy_out(step).wait()


def results(sources, token):
    piece = 128 * 2816 * 2
    kinds = []
    for r in sources:
        if (key := (r.shape[1:], r.dtype)) not in kinds:
            kinds.append(key)
    buffers = []
    for (_, width), dtype in kinds:
        buffers.append(pltpu.VMEM((SLOTS, piece // (width * dtype.itemsize), width), dtype))
    size = sum(r.size * r.dtype.itemsize for r in sources)
    return pl.pallas_call(
        functools.partial(results_kernel, len(sources), None),
        in_specs=[ANY] * (len(sources) + 1),
        out_specs=[ANY] * len(sources),
        out_shape=[jax.ShapeDtypeStruct(r.shape, r.dtype) for r in sources],
        scratch_shapes=buffers + [pltpu.SemaphoreType.DMA((len(kinds), SLOTS))] * 2,
        compiler_params=pltpu.CompilerParams(vmem_limit_bytes=62 * MIB),
        cost_estimate=pl.CostEstimate(flops=20 * 10**9, bytes_accessed=2 * size, transcendentals=0),
        name="results",
    )(*sources, token)


def kept_kernel(n, axis, blocks, away, *refs):
    halves, (ng_out, nu_out, nd_out, sem) = refs[: 2 * len(away)], refs[2 * len(away) + 3 :]
    q, u = BLOCK, UNIT
    small = q // 2
    pair = q + small
    me = lax.axis_index(axis)
    ff = nd_out.shape[1]
    mult = pl.multiple_of
    copies = []

    def put(src, dst):
        copies.append(pltpu.make_async_copy(src, dst, sem.at[len(copies)]))

    for k, src in enumerate(halves):
        dev, half = lax.rem(me + away[k // 2], n), k % 2
        base = dev * (ff // n)
        out = (ng_out, nu_out)[half]
        rows = pl.ds(mult(dev * q, q), q)
        for b in range(4):
            put(src.at[pl.ds(b * pair, q)], out.at[0, rows, pl.ds(block_of(blocks - 4 + b) * q, q)])
        for b in range(8):
            at_ = b * pair + q if b < 4 else 4 * pair + (b - 4) * small
            row = pl.ds(mult(base + b // 4 * 4 * u + dev * u + half * small, u), small)
            put(src.at[pl.ds(at_, small)], nd_out.at[0, row, pl.ds(b % 4 * q, q)])
    for c in copies:
        c.start()
    for c in copies:
        c.wait()


def place_kept(parts, away, weights, n, axis):
    blocks = weights[0].shape[-1] // BLOCK
    vmem = pl.BlockSpec(memory_space=pltpu.VMEM)
    count = len(parts)
    return pl.pallas_call(
        functools.partial(kept_kernel, n, axis, blocks, away),
        in_specs=[vmem] * count + [ANY] * 3,
        out_specs=[ANY] * 3,
        out_shape=[jax.ShapeDtypeStruct(w.shape, w.dtype) for w in weights],
        input_output_aliases={count + k: k for k in range(3)},
        scratch_shapes=[pltpu.SemaphoreType.DMA((count * 12,))],
        compiler_params=pltpu.CompilerParams(vmem_limit_bytes=62 * MIB),
        cost_estimate=pl.CostEstimate(flops=10**9, bytes_accessed=count * 4 * MIB, transcendentals=0),
        name="place_kept",
    )(*parts, *weights)


def solution(mesh):
    n = mesh.shape["dp"]
    to_right = [(k, (k + 1) % n) for k in range(n)]
    to_left = [(k, (k - 1) % n) for k in range(n)]

    def step(x, dy, wg, wu, wd, m_g, m_u, m_d, v_g, v_u, v_d):
        x, dy = x[0], dy[0]
        a0, h1, a1 = forward(x, wg, wu, wd)
        ng, nu, nd, mg, mu, md, vg, vu, vd, _, a, b = backward(a1, dy, h1, a0, wg, wu, wd, (m_g, m_u, m_d, v_g, v_u, v_d), n, "dp")
        la, rb = lax.ppermute(a, "dp", to_right), lax.ppermute(b, "dp", to_left)
        mg, mu, vg, vu = results((mg, mu, vg, vu), a)
        a, b, mg = lax.optimization_barrier((a, b, mg))
        lb, ra = lax.ppermute(b, "dp", to_right), lax.ppermute(a, "dp", to_left)
        md, vd, nd = results((md, vd, nd), mg)
        la, rb, md = lax.optimization_barrier((la, rb, md))
        fa, fb = lax.ppermute(la, "dp", to_right), lax.ppermute(rb, "dp", to_left)
        ng, nu = results((ng, nu), md)
        new = place_kept((a, b, ra, rb, la, lb), (0, 1, n - 1), (ng, nu, nd), n, "dp")
        new = place_kept((fa, fb), (2,), new, n, "dp")
        return (*new, mg, mu, md, vg, vu, vd)

    seq = P(("rep", "dp"), None, None)
    rows = P(None, "dp", None)
    whole = P("rep", None, None)
    part = P("rep", "dp", None)
    return jax.shard_map(
        step,
        mesh=mesh,
        in_specs=(seq, seq, P(), P(), P()) + (rows,) * 6,
        out_specs=(whole,) * 3 + (part,) * 6,
        check_vma=False,
    )
```
